8 devices in a mesh: col: 2 (over z, y), row: 4 (over x, core).
Axes of the slice: x: 2, y: 2, z: 1, core: 2. Of those that a mesh axis runs over, the one named last changes fastest.
Arguments:
- inter_mask: int32 [4096, 65536], P('row', 'col')
- emb_user: bfloat16 [4096, 64], P(('row', 'col'))
- emb_item: bfloat16 [65536, 64], P(('col', 'row'))
- triples: int32 [4096, 3], replicated
Outputs:
- output 1: bfloat16 [4096, 64], P(('row', 'col'))
- output 2: bfloat16 [65536, 64], P(('col', 'row'))
- output 3: float32 [4096], replicated
All inputs are finite; a program needn't handle non-finite values.
Results may differ from the reference program's by a relative error of at most 0.00805716.
Values are sent between devices in bfloat16 or wider.
A program may use at most 1 GiB of HBM per device.

```python
import jax
import jax.numpy as jnp
from jax import lax

EMB = 64
LAYERS = 3
USERS = 4096
ITEMS = 65536
BATCH = 4096
ACT_MAX = 8
DENS_DIV = 256


def draw_mask(base_key):
    key_user, key_item, key_edge = jax.random.split(base_key, 3)
    user_act = jax.random.randint(key_user, (USERS, 1), 1, ACT_MAX + 1)
    item_pop = jax.random.randint(key_item, (1, ITEMS), 1, ACT_MAX + 1)
    edge_draw = jax.random.randint(key_edge, (USERS, ITEMS), 0, DENS_DIV)
    return (edge_draw < user_act * item_pop).astype(jnp.int32)


def draw_triples(base_key):
    key_user, key_pos, key_neg = jax.random.split(base_key, 3)
    user_ids = jax.random.randint(key_user, (BATCH,), 0, USERS)
    pos_ids = jax.random.randint(key_pos, (BATCH,), 0, ITEMS)
    neg_ids = jax.random.randint(key_neg, (BATCH,), 0, ITEMS)
    return jnp.stack([user_ids, pos_ids, neg_ids], axis=1).astype(jnp.int32)


def setup_inputs(seed: int = 0) -> dict:
    sub_keys = jax.random.split(jax.random.key(seed), 8)
    user_mean = jax.random.normal(sub_keys[1], (1, EMB), jnp.float32)
    user_noise = jax.random.normal(sub_keys[2], (USERS, EMB), jnp.float32)
    user_walk = jnp.cumsum(jax.random.normal(sub_keys[6], (USERS, EMB), jnp.float32), axis=0) * (USERS ** -0.5)
    item_mean = jax.random.normal(sub_keys[3], (1, EMB), jnp.float32)
    item_noise = jax.random.normal(sub_keys[4], (ITEMS, EMB), jnp.float32)
    item_walk = jnp.cumsum(jax.random.normal(sub_keys[7], (ITEMS, EMB), jnp.float32), axis=0) * (ITEMS ** -0.5)
    return {
        "inter_mask": draw_mask(sub_keys[0]),
        "emb_user": (0.5 * (user_mean + user_noise + user_walk)).astype(jnp.bfloat16),
        "emb_item": (0.5 * (item_mean + item_noise + item_walk)).astype(jnp.bfloat16),
        "triples": draw_triples(sub_keys[5]),
    }


def reference(inter_mask, emb_user, emb_item, triples):
    deg_user = jnp.maximum(jnp.sum(inter_mask, axis=1), 1).astype(jnp.float32)
    deg_item = jnp.maximum(jnp.sum(inter_mask, axis=0), 1).astype(jnp.float32)
    adj_norm = (inter_mask.astype(jnp.float32) * lax.rsqrt(deg_user)[:, None] * lax.rsqrt(deg_item)[None, :]).astype(jnp.bfloat16)

    def layer_step(carry, unused):
        cur_user, cur_item, total_user, total_item = carry
        next_user = jnp.dot(adj_norm, cur_item, preferred_element_type=jnp.float32).astype(jnp.bfloat16)
        next_item = jnp.dot(adj_norm.T, cur_user, preferred_element_type=jnp.float32).astype(jnp.bfloat16)
        new_carry = (next_user, next_item, total_user + next_user.astype(jnp.float32), total_item + next_item.astype(jnp.float32))
        return new_carry, None

    start_carry = (emb_user, emb_item, emb_user.astype(jnp.float32), emb_item.astype(jnp.float32))
    final_carry, unused_out = lax.scan(layer_step, start_carry, None, length=LAYERS)
    out_user = (final_carry[2] / (LAYERS + 1)).astype(jnp.bfloat16)
    out_item = (final_carry[3] / (LAYERS + 1)).astype(jnp.bfloat16)
    vec_user = out_user[triples[:, 0]].astype(jnp.float32)
    vec_pos = out_item[triples[:, 1]].astype(jnp.float32)
    vec_neg = out_item[triples[:, 2]].astype(jnp.float32)
    margin = jnp.sum(vec_user * vec_pos, axis=1) - jnp.sum(vec_user * vec_neg, axis=1)
    bpr_loss = jax.nn.softplus(-margin)
    return out_user, out_item, bpr_loss
```

```python
import jax
import jax.numpy as jnp
from jax import lax
from jax.experimental import pallas as pl
from jax.experimental.pallas import tpu as pltpu
from jax.sharding import PartitionSpec as P

LAYERS = 3
F8 = jnp.float8_e4m3fn
BF = jnp.bfloat16
F32 = jnp.float32
MESH = pl.DeviceIdType.MESH

EMB = 64
USERS = 1024
HALF = 512
QUART = 8192
CH = 1024
NCH = 8
NBLK = 32
PIECE = 256
RING = 7
UP_U, DN_U = 256.0, 1.0 / 256.0
UP_I, DN_I = 64.0, 1.0 / 64.0
LAG_B, LAG_C, LAG_D = 2, 3, 4


def _scale(val, s8):
    rows, cols = val.shape
    return (val.reshape(rows // 8, 8, cols) * s8[None]).reshape(rows, cols)


def _main_kernel(mask, eu0, ei0, out_i, ua,
                 m8, stage, pan, snd_a, rcv_a, snd_b, rcv_b, xs, xr,
                 uacc, yr, raw, eus, cs, csr, sib, cacc, rs, rsum, rsum_r, su,
                 st_sem, ld_sem, agx_s, agx_r, agd_s, agd_r, agf_s, agf_r, cs_s, cs_r,
                 rs_s, rs_r, a_s, a_r, b_s, b_r, x_s, x_r, y_s, y_r, w_s, w_r, g_s, g_r):
    c = lax.axis_index("col")
    r = lax.axis_index("row")
    x = r // 2
    k = r % 2
    r_par = 2 * x + (1 - k)
    r_xp = 2 * (1 - x) + k
    r_xq = 2 * (1 - x) + (1 - k)
    par = (c, r_par)
    xpe = (c, r_xp)
    xpa = (c, r_xq)
    ype = (1 - c, r)

    def rcopy(src, dst, ss, rsm, dev):
        return pltpu.make_async_remote_copy(src_ref=src, dst_ref=dst, send_sem=ss, recv_sem=rsm,
                                            device_id=dev, device_id_type=MESH)

    def piece(p):
        blk = p // 4
        row = pl.multiple_of((p % 4) * PIECE, PIECE)
        col = pl.multiple_of((blk % 4) * QUART + (blk // 4) * CH, CH)
        return pltpu.make_async_copy(mask.at[pl.ds(row, PIECE), pl.ds(col, CH)],
                                     stage.at[p % RING], st_sem.at[p % RING])

    for p in range(RING):
        piece(p).start()

    def own_load(j):
        return pltpu.make_async_copy(ei0.at[:, pl.ds(pl.multiple_of(j * CH, CH), CH)],
                                     pan.at[0, j * 4 + r], ld_sem.at[j])

    user_load = pltpu.make_async_copy(eu0, raw.at[0, c], ld_sem.at[NCH])
    for j in range(NCH):
        own_load(j).start()
    user_load.start()

    barrier = pltpu.get_barrier_semaphore()
    for cc in range(2):
        for rr in range(4):
            pl.semaphore_signal(barrier, inc=1, device_id=(cc, rr), device_id_type=MESH)
    pl.semaphore_wait(barrier, 8)

    def ag_x(a, j, q):
        i = a * NCH + j
        ref = pan.at[a, j * 4 + q]
        return rcopy(ref, ref, agx_s.at[i], agx_r.at[i], xpe)

    def ag_d(a, j, q):
        i = a * NCH + j
        ref = pan.at[a, j * 4 + q]
        return rcopy(ref, ref, agd_s.at[i], agd_r.at[i], par)

    def ag_f(a, j, q):
        i = a * NCH + j
        ref = pan.at[a, j * 4 + q]
        return rcopy(ref, ref, agf_s.at[i], agf_r.at[i], par)

    for j in range(NCH):
        own_load(j).wait()
        ag_x(0, j, r).start()
        ag_d(0, j, r).start()
    user_load.wait()
    w0 = rcopy(raw.at[0, c], raw.at[0, c], w_s.at[0], w_r.at[0], ype)
    w0.start()

    rs[...] = jnp.zeros_like(rs)
    uacc[...] = jnp.zeros_like(uacc)

    def cs_copy(rel, g, dev):
        return rcopy(cs.at[pl.ds(g * 4, 4)], csr.at[rel, pl.ds(g * 4, 4)], cs_s.at[rel, g], cs_r.at[rel, g], dev)

    def user_prod(a, b):
        es = _scale(pan[a, b].astype(F32), sib[b] * DN_U).astype(BF)
        got = lax.dot_general(es, m8[b], (((1,), (1,)), ((), ())), preferred_element_type=F32)
        uacc[0] += got[:, :HALF]
        uacc[1] += got[:, HALF:]

    def first_users(g):
        for rel, dev in ((0, par), (1, xpe), (2, xpa)):
            cs_copy(rel, g, dev).wait_recv()
        ag_d(0, g, r_par).wait_recv()
        ag_f(0, g, r_xq).wait_recv()

        @pl.loop(0, 4)
        def _(q):
            b = g * 4 + q
            deg = cs[b] + csr[0, b] + csr[1, b] + csr[2, b]
            sib[b] = jnp.broadcast_to(lax.rsqrt(jnp.maximum(deg, 1.0)), (8, CH))
            user_prod(0, b)

    @pl.loop(0, NCH)
    def _(g):
        @pl.loop(0, 4)
        def _(q):
            b = g * 4 + q
            cacc[...] = jnp.zeros_like(cacc)

            @pl.loop(0, 4)
            def _(s):
                p = b * 4 + s
                piece(p).wait()
                slot = p % RING

                @pl.loop(0, PIECE // 32)
                def _(i):
                    rows = pl.ds(pl.multiple_of(i * 32, 32), 32)
                    dst = pl.ds(pl.multiple_of(s * PIECE + i * 32, 32), 32)
                    f = stage[slot, rows, :].astype(F32)
                    m8[b, dst, :] = f.astype(F8)
                    cacc[...] += jnp.sum(f.reshape(4, 8, CH), axis=0)
                    part = f[:, :128]
                    for w in range(1, CH // 128):
                        part = part + f[:, w * 128:(w + 1) * 128]
                    rs[dst, :] += part

                @pl.when(p + RING < 4 * NBLK)
                def _():
                    piece(p + RING).start()

            cs[b] = jnp.sum(cacc[...], axis=0, keepdims=True)

        for rel, dev in ((0, par), (1, xpe), (2, xpa)):
            cs_copy(rel, g, dev).start()
        ag_x(0, g, r_xp).wait_recv()
        ag_f(0, g, r_xp).start()

        @pl.when(g >= 1)
        def _():
            first_users(g - 1)

    rsum[...] = lax.dot_general(jnp.ones((8, 128), BF), rs[...].astype(BF), (((1,), (1,)), ((), ())),
                                preferred_element_type=F32)
    rs_copy = rcopy(rsum, rsum_r, rs_s.at[0], rs_r.at[0], ype)
    rs_copy.start()
    first_users(NCH - 1)
    rs_copy.wait()
    w0.wait()
    deg_u = lax.rsqrt(jnp.maximum(rsum[...] + rsum_r[...], 1.0))
    su[0] = deg_u[:, :HALF]
    su[1] = deg_u[:, HALF:]

    def user_operand(lay):
        for h in range(2):
            eus[lay, :, h * HALF:(h + 1) * HALF] = _scale(raw[lay, h].astype(F32), su[h] * DN_I).astype(BF)

    user_operand(0)

    def prod(lay, b):
        return jnp.dot(eus[lay], m8[b], preferred_element_type=F32)

    def cp_a(g):
        return rcopy(snd_a.at[g % 2], rcv_a.at[g % 2], a_s.at[g % 2], a_r.at[g % 2], par)

    def cp_b(g):
        return rcopy(snd_b.at[g % 4], rcv_b.at[g % 4], b_s.at[g % 4], b_r.at[g % 4], par)

    def cp_x(g):
        return rcopy(xs.at[g % 4], xr.at[g % 8], x_s.at[g % 4], x_r.at[g % 8], xpe)

    def step_a(g):
        lay = g // NCH
        b = (g % NCH) * 4

        @pl.when(g >= 2)
        def _():
            cp_a(g - 2).wait_send()

        snd_a[g % 2] = prod(lay, b + r_xq)
        cp_a(g).start()

        @pl.when(g >= 4)
        def _():
            cp_x(g - 4).wait_send()

        xs[g % 4] = prod(lay, b + r_xp)
        cp_a(g).wait_recv()
        xs[g % 4] += rcv_a[g % 2]
        cp_x(g).start()

        @pl.when(g >= 4)
        def _():
            cp_b(g - 4).wait_send()

        snd_b[g % 4] = prod(lay, b + r_par)
        cp_b(g).start()

    def step_b(g):
        lay = g // NCH
        j = g % NCH
        b = j * 4 + r
        own = prod(lay, b)
        cp_b(g).wait_recv()
        own = own + rcv_b[g % 4]
        cp_x(g).wait_recv()
        emb = _scale(own + xr[g % 8], sib[b] * UP_I).astype(BF)

        @pl.when(lay < 2)
        def _():
            pan[lay + 1, b] = emb
            ag_x(lay + 1, j, r).start()
            ag_d(lay + 1, j, r).start()

        @pl.when(lay == 2)
        def _():
            tot = pan[0, b].astype(F32) + pan[1, b].astype(F32) + pan[2, b].astype(F32) + emb.astype(F32)
            out_i[:, pl.ds(pl.multiple_of(j * CH, CH), CH)] = (tot * 0.25).astype(BF)

    def step_c(g):
        a = g // NCH + 1
        ag_x(a, g % NCH, r_xp).wait_recv()
        ag_f(a, g % NCH, r_xp).start()

    def step_d(g):
        a = g // NCH + 1
        j = g % NCH
        ag_d(a, j, r_par).wait_recv()
        ag_f(a, j, r_xq).wait_recv()

        @pl.loop(0, 4)
        def _(q):
            user_prod(a, j * 4 + q)

    def cp_y(lay):
        return rcopy(uacc.at[1 - c], yr.at[lay - 1], y_s.at[lay - 1], y_r.at[lay - 1], ype)

    def cp_w(lay):
        return rcopy(raw.at[lay, c], raw.at[lay, c], w_s.at[lay], w_r.at[lay], ype)

    def user_emb(lay):
        cp_y(lay).wait()
        emb = _scale(uacc[c] + yr[lay - 1], su[c] * UP_U).astype(BF)
        uacc[...] = jnp.zeros_like(uacc)
        return emb

    def finish_user(lay):
        raw[lay, c] = user_emb(lay)
        cp_w(lay).start()

    def load_user(lay):
        cp_w(lay).wait()
        user_operand(lay)

    def cp_g(i, blk, dev):
        return rcopy(ua.at[blk], ua.at[blk], g_s.at[i], g_r.at[i], dev)

    own_u = 2 * r + c
    D1, D2 = NCH - 1 + LAG_D, 2 * NCH - 1 + LAG_D

    @pl.loop(0, LAYERS * NCH + LAG_B)
    def _(t):
        @pl.when(t < LAYERS * NCH)
        def _():
            step_a(t)

        @pl.when(t == 0)
        def _():
            cp_y(1).start()

        @pl.when(t == 1)
        def _():
            finish_user(1)

        @pl.when(t == 2)
        def _():
            load_user(1)

        @pl.when(t == D1 + 1)
        def _():
            finish_user(2)

        @pl.when(t == D1 + 2)
        def _():
            load_user(2)

        @pl.when(t == D2 + 1)
        def _():
            emb = user_emb(3).astype(F32)
            tot = raw[0, c].astype(F32) + raw[1, c].astype(F32) + raw[2, c].astype(F32) + emb
            ua[own_u] = (tot * 0.25).astype(BF)
            cp_g(0, own_u, ype).start()
            cp_g(1, own_u, par).start()
            cp_g(2, own_u, xpe).start()

        @pl.when(t == D2 + 2)
        def _():
            cp_g(0, 2 * r + 1 - c, ype).wait_recv()
            cp_g(1, 2 * r_par + c, par).wait_recv()
            cp_g(2, 2 * r_xp + c, xpe).wait_recv()
            cp_g(3, 2 * r + 1 - c, par).start()
            cp_g(4, 2 * r_xp + c, par).start()
            cp_g(5, 2 * r_xp + c, ype).start()

        @pl.when(t == D2 + 3)
        def _():
            cp_g(3, 2 * r_par + 1 - c, par).wait_recv()
            cp_g(4, 2 * r_xq + c, par).wait_recv()
            cp_g(5, 2 * r_xp + 1 - c, ype).wait_recv()
            cp_g(6, 2 * r_xp + 1 - c, par).start()

        @pl.when(t == D2 + 4)
        def _():
            cp_g(6, 2 * r_xq + 1 - c, par).wait_recv()

        @pl.when(t >= LAG_B)
        def _():
            step_b(t - LAG_B)

        @pl.when((t >= LAG_C) & (t < 2 * NCH + LAG_C))
        def _():
            step_c(t - LAG_C)

        @pl.when((t >= LAG_D) & (t < 2 * NCH + LAG_D))
        def _():
            step_d(t - LAG_D)

        @pl.when(t == D1)
        def _():
            cp_y(2).start()

        @pl.when(t == D2)
        def _():
            cp_y(3).start()

    last = LAYERS * NCH
    for g in range(last - 2, last):
        cp_a(g).wait_send()
    for g in range(last - 4, last):
        cp_b(g).wait_send()
    for g in range(last - 4, last):
        cp_x(g).wait_send()
    for i in range(7):
        cp_g(i, own_u, par).wait_send()

    @pl.loop(0, NCH)
    def _(j):
        for rel, dev in ((0, par), (1, xpe), (2, xpa)):
            cs_copy(rel, j, dev).wait_send()

    @pl.loop(0, 3 * NCH)
    def _(i):
        ag_x(i // NCH, i % NCH, r).wait_send()
        ag_d(i // NCH, i % NCH, r).wait_send()
        ag_f(i // NCH, i % NCH, r_xp).wait_send()


def _main(mask, eu0, ei0):
    dma = pltpu.SemaphoreType.DMA
    any_spec = pl.BlockSpec(memory_space=pl.ANY)
    vmem = pl.BlockSpec(memory_space=pltpu.VMEM)
    return pl.pallas_call(
        _main_kernel,
        out_shape=(jax.ShapeDtypeStruct((EMB, QUART), BF), jax.ShapeDtypeStruct((8, EMB, HALF), BF)),
        in_specs=[any_spec, any_spec, any_spec],
        out_specs=(vmem, vmem),
        scratch_shapes=[
            pltpu.VMEM((NBLK, USERS, CH), F8),
            pltpu.VMEM((RING, PIECE, CH), jnp.int32),
            pltpu.VMEM((3, NBLK, EMB, CH), BF),
            pltpu.VMEM((2, EMB, CH), F32), pltpu.VMEM((2, EMB, CH), F32),
            pltpu.VMEM((4, EMB, CH), F32), pltpu.VMEM((4, EMB, CH), F32),
            pltpu.VMEM((4, EMB, CH), F32), pltpu.VMEM((8, EMB, CH), F32),
            pltpu.VMEM((2, EMB, HALF), F32), pltpu.VMEM((3, EMB, HALF), F32),
            pltpu.VMEM((3, 2, EMB, HALF), BF), pltpu.VMEM((3, EMB, USERS), BF),
            pltpu.VMEM((NBLK, 1, CH), F32), pltpu.VMEM((3, NBLK, 1, CH), F32),
            pltpu.VMEM((NBLK, 8, CH), F32), pltpu.VMEM((8, CH), F32),
            pltpu.VMEM((USERS, 128), F32), pltpu.VMEM((8, USERS), F32), pltpu.VMEM((8, USERS), F32),
            pltpu.VMEM((2, 8, HALF), F32),
            dma((RING,)), dma((NCH + 1,)),
            dma((3 * NCH,)), dma((3 * NCH,)), dma((3 * NCH,)), dma((3 * NCH,)), dma((3 * NCH,)), dma((3 * NCH,)),
            dma((3, NCH)), dma((3, NCH)), dma((1,)), dma((1,)),
            dma((2,)), dma((2,)), dma((4,)), dma((4,)), dma((4,)), dma((8,)),
            dma((3,)), dma((3,)), dma((3,)), dma((3,)), dma((7,)), dma((7,)),
        ],
        compiler_params=pltpu.CompilerParams(collective_id=0, has_side_effects=True, vmem_limit_bytes=67043328),
        name="propagate",
    )(mask, eu0, ei0)


def _lookup_kernel(uid, pid, nid, items, users, own_p, own_n, out, it, ut, pp, pn):
    for i in range(QUART // 512):
        it[i * 512:(i + 1) * 512, :EMB] = items[:, i * 512:(i + 1) * 512].astype(F32).T
    for i in range(8):
        ut[i * HALF:(i + 1) * HALF, :EMB] = users[i].astype(F32).T

    @pl.loop(0, 4096 // 16)
    def _(i):
        for w in range(16):
            t = i * 16 + w
            u = ut[pl.ds(uid[t], 1), :]
            pp[pl.ds(t, 1), :] = u * it[pl.ds(pid[t], 1), :]
            pn[pl.ds(t, 1), :] = u * it[pl.ds(nid[t], 1), :]

    @pl.loop(0, 32)
    def _(i):
        rows = pl.ds(pl.multiple_of(i * 128, 128), 128)
        sp = jnp.sum(pp[rows, :].T[:EMB], axis=0, keepdims=True)
        sn = jnp.sum(pn[rows, :].T[:EMB], axis=0, keepdims=True)
        row = pl.ds(i, 1)
        out[row, :] = (jnp.where(own_p[row, :] > 0, sp, 0.0) - jnp.where(own_n[row, :] > 0, sn, 0.0))


def _lookup(uid, pid, nid, items, users, own_p, own_n):
    vmem = pl.BlockSpec(memory_space=pltpu.VMEM)
    smem = pl.BlockSpec(memory_space=pltpu.SMEM)
    return pl.pallas_call(
        _lookup_kernel,
        out_shape=jax.ShapeDtypeStruct((32, 128), F32),
        in_specs=[smem, smem, smem, vmem, vmem, vmem, vmem],
        out_specs=vmem,
        scratch_shapes=[pltpu.VMEM((QUART, 128), F32), pltpu.VMEM((4096, 128), F32),
                        pltpu.VMEM((4096, 128), F32), pltpu.VMEM((4096, 128), F32)],
        name="lookup",
    )(uid, pid, nid, items, users, own_p, own_n)


def _loss_kernel(part, out, got, s_sem, r_sem):
    c = lax.axis_index("col")
    r = lax.axis_index("row")
    me = 2 * r + c
    barrier = pltpu.get_barrier_semaphore()
    for cc in range(2):
        for rr in range(4):
            pl.semaphore_signal(barrier, inc=1, device_id=(cc, rr), device_id_type=MESH)
    pl.semaphore_wait(barrier, 8)

    def copy(i, slot):
        dr, dc = i // 2, i % 2
        return pltpu.make_async_remote_copy(
            src_ref=part, dst_ref=got.at[slot], send_sem=s_sem.at[i], recv_sem=r_sem.at[i],
            device_id=((c + dc) % 2, (r + dr) % 4), device_id_type=MESH)

    def sender(i):
        return 2 * ((r + 4 - i // 2) % 4) + (c + i % 2) % 2

    for i in range(1, 8):
        copy(i, me).start()
    got[me] = part[...]
    for i in range(1, 8):
        copy(i, sender(i)).wait()
    m = got[0]
    for i in range(1, 8):
        m = m + got[i]
    out[...] = jnp.maximum(-m, 0.0) + jnp.log1p(jnp.exp(-jnp.abs(m)))


def _loss(part):
    vmem = pl.BlockSpec(memory_space=pltpu.VMEM)
    return pl.pallas_call(
        _loss_kernel,
        out_shape=jax.ShapeDtypeStruct((32, 128), F32),
        in_specs=[vmem],
        out_specs=vmem,
        scratch_shapes=[pltpu.VMEM((8, 32, 128), F32), pltpu.SemaphoreType.DMA((8,)), pltpu.SemaphoreType.DMA((8,))],
        compiler_params=pltpu.CompilerParams(collective_id=1, has_side_effects=True),
        name="loss",
    )(part)


def solution(mesh):
    def device_body(mask_blk, user_shard, item_shard, triples):
        row_idx = lax.axis_index("row")
        col_idx = lax.axis_index("col")
        out_it, users = _main(mask_blk, user_shard.T, item_shard.T)
        me = 2 * row_idx + col_idx
        out_ut = lax.dynamic_index_in_dim(users, me, 0, keepdims=False)
        start = (col_idx * 4 + row_idx) * QUART
        uid, pid, nid = triples[:, 0], triples[:, 1] - start, triples[:, 2] - start
        own_p = ((pid >= 0) & (pid < QUART)).astype(jnp.int32).reshape(32, 128)
        own_n = ((nid >= 0) & (nid < QUART)).astype(jnp.int32).reshape(32, 128)
        part = _lookup(uid, jnp.clip(pid, 0, QUART - 1), jnp.clip(nid, 0, QUART - 1), out_it, users, own_p, own_n)
        bpr_loss = _loss(part).reshape(4096)
        return out_ut.T, out_it.T, bpr_loss

    return jax.shard_map(
        device_body,
        mesh=mesh,
        in_specs=(P("row", "col"), P(("row", "col"), None), P(("col", "row"), None), P()),
        out_specs=(P(("row", "col"), None), P(("col", "row"), None), P()),
        check_vma=False,
    )
```

```python
import jax
import jax.numpy as jnp
from jax import lax
from jax.experimental import pallas as pl
from jax.experimental.pallas import tpu as pltpu
from jax.sharding import PartitionSpec as P

LAYERS = 3
F8 = jnp.float8_e4m3fn
BF = jnp.bfloat16
F32 = jnp.float32
MESH = pl.DeviceIdType.MESH

EMB = 64
USERS = 1024
HALF = 512
QUART = 8192
CH = 1024
NCH = 8
NBLK = 32
PIECE = 256
RING = 7
UP_U, DN_U = 256.0, 1.0 / 256.0
UP_I, DN_I = 64.0, 1.0 / 64.0
LAG_B, LAG_C, LAG_D = 2, 3, 4
AHEAD = 2


def _scale(val, s8):
    rows, cols = val.shape
    return (val.reshape(rows // 8, 8, cols) * s8[None]).reshape(rows, cols)


def _main_kernel(mask, eu0, ei0, out_i, ua,
                 m8, stage, pan, snd_a, rcv_a, snd_b, rcv_b, xs, xr,
                 uacc, yr, raw, eus, cs, csr, sib, cacc, rs, rsum, rsum_r, su,
                 st_sem, ld_sem, agx_s, agx_r, agd_s, agd_r, agf_s, agf_r, cs_s, cs_r,
                 rs_s, rs_r, a_s, a_r, b_s, b_r, x_s, x_r, y_s, y_r, w_s, w_r, g_s, g_r):
    c = lax.axis_index("col")
    r = lax.axis_index("row")
    x = r // 2
    k = r % 2
    r_par = 2 * x + (1 - k)
    r_xp = 2 * (1 - x) + k
    r_xq = 2 * (1 - x) + (1 - k)
    par = (c, r_par)
    xpe = (c, r_xp)
    xpa = (c, r_xq)
    ype = (1 - c, r)

    def rcopy(src, dst, ss, rsm, dev):
        return pltpu.make_async_remote_copy(src_ref=src, dst_ref=dst, send_sem=ss, recv_sem=rsm,
                                            device_id=dev, device_id_type=MESH)

    def piece(p):
        blk = p // 4
        row = pl.multiple_of((p % 4) * PIECE, PIECE)
        col = pl.multiple_of((blk % 4) * QUART + (blk // 4) * CH, CH)
        return pltpu.make_async_copy(mask.at[pl.ds(row, PIECE), pl.ds(col, CH)],
                                     stage.at[p % RING], st_sem.at[p % RING])

    for p in range(RING):
        piece(p).start()

    def own_load(j):
        return pltpu.make_async_copy(ei0.at[:, pl.ds(pl.multiple_of(j * CH, CH), CH)],
                                     pan.at[0, j * 4 + r], ld_sem.at[j])

    user_load = pltpu.make_async_copy(eu0, raw.at[0, c], ld_sem.at[NCH])
    for j in range(NCH):
        own_load(j).start()
    user_load.start()

    barrier = pltpu.get_barrier_semaphore()
    for cc in range(2):
        for rr in range(4):
            pl.semaphore_signal(barrier, inc=1, device_id=(cc, rr), device_id_type=MESH)
    pl.semaphore_wait(barrier, 8)

    def ag_x(a, j, q):
        i = a * NCH + j
        ref = pan.at[a, j * 4 + q]
        return rcopy(ref, ref, agx_s.at[i], agx_r.at[i], xpe)

    def ag_d(a, j, q):
        i = a * NCH + j
        ref = pan.at[a, j * 4 + q]
        return rcopy(ref, ref, agd_s.at[i], agd_r.at[i], par)

    def ag_f(a, j, q):
        i = a * NCH + j
        ref = pan.at[a, j * 4 + q]
        return rcopy(ref, ref, agf_s.at[i], agf_r.at[i], par)

    for j in range(NCH):
        own_load(j).wait()
        if j < AHEAD:
            ag_x(0, j, r).start()
        ag_d(0, j, r).start()
    user_load.wait()
    w0 = rcopy(raw.at[0, c], raw.at[0, c], w_s.at[0], w_r.at[0], ype)
    w0.start()

    rs[...] = jnp.zeros_like(rs)
    uacc[...] = jnp.zeros_like(uacc)

    def cs_copy(rel, g, dev):
        return rcopy(cs.at[pl.ds(g * 4, 4)], csr.at[rel, pl.ds(g * 4, 4)], cs_s.at[rel, g], cs_r.at[rel, g], dev)

    def user_prod(a, b):
        es = _scale(pan[a, b].astype(F32), sib[b] * DN_U).astype(BF)
        got = lax.dot_general(es, m8[b], (((1,), (1,)), ((), ())), preferred_element_type=F32)
        uacc[0] += got[:, :HALF]
        uacc[1] += got[:, HALF:]

    def first_users(g):
        for rel, dev in ((0, par), (1, xpe), (2, xpa)):
            cs_copy(rel, g, dev).wait_recv()
        ag_d(0, g, r_par).wait_recv()
        ag_f(0, g, r_xq).wait_recv()

        @pl.loop(0, 4)
        def _(q):
            b = g * 4 + q
            deg = cs[b] + csr[0, b] + csr[1, b] + csr[2, b]
            sib[b] = jnp.broadcast_to(lax.rsqrt(jnp.maximum(deg, 1.0)), (8, CH))
            user_prod(0, b)

    cp_deg = rcopy(rsum, rsum_r, rs_s.at[0], rs_r.at[0], ype)

    @pl.loop(0, NCH)
    def _(g):
        @pl.loop(0, 4)
        def _(q):
            b = g * 4 + q
            cacc[...] = jnp.zeros_like(cacc)

            @pl.loop(0, 4)
            def _(s):
                p = b * 4 + s
                piece(p).wait()
                slot = p % RING

                @pl.loop(0, PIECE // 32)
                def _(i):
                    rows = pl.ds(pl.multiple_of(i * 32, 32), 32)
                    dst = pl.ds(pl.multiple_of(s * PIECE + i * 32, 32), 32)
                    f = stage[slot, rows, :].astype(F32)
                    m8[b, dst, :] = f.astype(F8)
                    cacc[...] += jnp.sum(f.reshape(4, 8, CH), axis=0)
                    part = f[:, :128]
                    for w in range(1, CH // 128):
                        part = part + f[:, w * 128:(w + 1) * 128]
                    rs[dst, :] += part

                @pl.when(p + RING < 4 * NBLK)
                def _():
                    piece(p + RING).start()

            cs[b] = jnp.sum(cacc[...], axis=0, keepdims=True)

        for rel, dev in ((0, par), (1, xpe), (2, xpa)):
            cs_copy(rel, g, dev).start()

        @pl.when(g + AHEAD < NCH)
        def _():
            ag_x(0, g + AHEAD, r).start()

        @pl.when(g == NCH - 1)
        def _():
            rsum[...] = lax.dot_general(jnp.ones((8, 128), BF), rs[...].astype(BF), (((1,), (1,)), ((), ())),
                                        preferred_element_type=F32)
            cp_deg.start()

        ag_x(0, g, r_xp).wait_recv()
        ag_f(0, g, r_xp).start()

        @pl.when((g >= 1) & (g < NCH - 1))
        def _():
            first_users(g - 1)

    cp_deg.wait()
    w0.wait()
    deg_u = lax.rsqrt(jnp.maximum(rsum[...] + rsum_r[...], 1.0))
    su[0] = deg_u[:, :HALF]
    su[1] = deg_u[:, HALF:]

    def user_operand(lay):
        for h in range(2):
            eus[lay, :, h * HALF:(h + 1) * HALF] = _scale(raw[lay, h].astype(F32), su[h] * DN_I).astype(BF)

    user_operand(0)

    def prod(lay, b):
        return jnp.dot(eus[lay], m8[b], preferred_element_type=F32)

    def cp_a(g):
        return rcopy(snd_a.at[g % 2], rcv_a.at[g % 2], a_s.at[g % 2], a_r.at[g % 2], par)

    def cp_b(g):
        return rcopy(snd_b.at[g % 4], rcv_b.at[g % 4], b_s.at[g % 4], b_r.at[g % 4], par)

    def cp_x(g):
        return rcopy(xs.at[g % 4], xr.at[g % 8], x_s.at[g % 4], x_r.at[g % 8], xpe)

    def step_a(g):
        lay = g // NCH
        b = (g % NCH) * 4

        @pl.when(g >= 2)
        def _():
            cp_a(g - 2).wait_send()

        snd_a[g % 2] = prod(lay, b + r_xq)
        cp_a(g).start()

        @pl.when(g >= 4)
        def _():
            cp_x(g - 4).wait_send()

        xs[g % 4] = prod(lay, b + r_xp)
        cp_a(g).wait_recv()
        xs[g % 4] += rcv_a[g % 2]
        cp_x(g).start()

        @pl.when(g >= 4)
        def _():
            cp_b(g - 4).wait_send()

        snd_b[g % 4] = prod(lay, b + r_par)
        cp_b(g).start()

    def step_b(g):
        lay = g // NCH
        j = g % NCH
        b = j * 4 + r
        own = prod(lay, b)
        cp_b(g).wait_recv()
        own = own + rcv_b[g % 4]
        cp_x(g).wait_recv()
        emb = _scale(own + xr[g % 8], sib[b] * UP_I).astype(BF)

        @pl.when(lay < 2)
        def _():
            pan[lay + 1, b] = emb
            ag_x(lay + 1, j, r).start()
            ag_d(lay + 1, j, r).start()

        @pl.when(lay == 2)
        def _():
            tot = pan[0, b].astype(F32) + pan[1, b].astype(F32) + pan[2, b].astype(F32) + emb.astype(F32)
            out_i[:, pl.ds(pl.multiple_of(j * CH, CH), CH)] = (tot * 0.25).astype(BF)

    def step_c(g):
        a = g // NCH + 1
        ag_x(a, g % NCH, r_xp).wait_recv()
        ag_f(a, g % NCH, r_xp).start()

    def step_d(g):
        a = g // NCH + 1
        j = g % NCH
        ag_d(a, j, r_par).wait_recv()
        ag_f(a, j, r_xq).wait_recv()

        @pl.loop(0, 4)
        def _(q):
            user_prod(a, j * 4 + q)

    def cp_y(lay):
        return rcopy(uacc.at[1 - c], yr.at[lay - 1], y_s.at[lay - 1], y_r.at[lay - 1], ype)

    def cp_w(lay):
        return rcopy(raw.at[lay, c], raw.at[lay, c], w_s.at[lay], w_r.at[lay], ype)

    def user_emb(lay):
        cp_y(lay).wait()
        emb = _scale(uacc[c] + yr[lay - 1], su[c] * UP_U).astype(BF)
        uacc[...] = jnp.zeros_like(uacc)
        return emb

    def finish_user(lay):
        raw[lay, c] = user_emb(lay)
        cp_w(lay).start()

    def load_user(lay):
        cp_w(lay).wait()
        user_operand(lay)

    def cp_g(i, blk, dev):
        return rcopy(ua.at[blk], ua.at[blk], g_s.at[i], g_r.at[i], dev)

    own_u = 2 * r + c
    D1, D2 = NCH - 1 + LAG_D, 2 * NCH - 1 + LAG_D

    @pl.loop(0, LAYERS * NCH + LAG_B)
    def _(t):
        @pl.when(t < LAYERS * NCH)
        def _():
            step_a(t)

        @pl.when(t < 2)
        def _():
            first_users(NCH - 2 + t)

        @pl.when(t == 1)
        def _():
            cp_y(1).start()

        @pl.when(t == 2)
        def _():
            finish_user(1)

        @pl.when(t == 3)
        def _():
            load_user(1)

        @pl.when(t == D1 + 1)
        def _():
            finish_user(2)

        @pl.when(t == D1 + 2)
        def _():
            load_user(2)

        @pl.when(t == D2 + 1)
        def _():
            emb = user_emb(3).astype(F32)
            tot = raw[0, c].astype(F32) + raw[1, c].astype(F32) + raw[2, c].astype(F32) + emb
            ua[own_u] = (tot * 0.25).astype(BF)
            cp_g(0, own_u, ype).start()
            cp_g(1, own_u, par).start()
            cp_g(2, own_u, xpe).start()

        @pl.when(t == D2 + 2)
        def _():
            cp_g(0, 2 * r + 1 - c, ype).wait_recv()
            cp_g(1, 2 * r_par + c, par).wait_recv()
            cp_g(2, 2 * r_xp + c, xpe).wait_recv()
            cp_g(3, 2 * r + 1 - c, par).start()
            cp_g(4, 2 * r_xp + c, par).start()
            cp_g(5, 2 * r_xp + c, ype).start()

        @pl.when(t == D2 + 3)
        def _():
            cp_g(3, 2 * r_par + 1 - c, par).wait_recv()
            cp_g(4, 2 * r_xq + c, par).wait_recv()
            cp_g(5, 2 * r_xp + 1 - c, ype).wait_recv()
            cp_g(6, 2 * r_xp + 1 - c, par).start()

        @pl.when(t == D2 + 4)
        def _():
            cp_g(6, 2 * r_xq + 1 - c, par).wait_recv()

        @pl.when(t >= LAG_B)
        def _():
            step_b(t - LAG_B)

        @pl.when((t >= LAG_C) & (t < 2 * NCH + LAG_C))
        def _():
            step_c(t - LAG_C)

        @pl.when((t >= LAG_D) & (t < 2 * NCH + LAG_D))
        def _():
            step_d(t - LAG_D)

        @pl.when(t == D1)
        def _():
            cp_y(2).start()

        @pl.when(t == D2)
        def _():
            cp_y(3).start()

    last = LAYERS * NCH
    for g in range(last - 2, last):
        cp_a(g).wait_send()
    for g in range(last - 4, last):
        cp_b(g).wait_send()
    for g in range(last - 4, last):
        cp_x(g).wait_send()
    for i in range(7):
        cp_g(i, own_u, par).wait_send()

    @pl.loop(0, NCH)
    def _(j):
        for rel, dev in ((0, par), (1, xpe), (2, xpa)):
            cs_copy(rel, j, dev).wait_send()

    @pl.loop(0, 3 * NCH)
    def _(i):
        ag_x(i // NCH, i % NCH, r).wait_send()
        ag_d(i // NCH, i % NCH, r).wait_send()
        ag_f(i // NCH, i % NCH, r_xp).wait_send()


def _main(mask, eu0, ei0):
    dma = pltpu.SemaphoreType.DMA
    any_spec = pl.BlockSpec(memory_space=pl.ANY)
    vmem = pl.BlockSpec(memory_space=pltpu.VMEM)
    return pl.pallas_call(
        _main_kernel,
        out_shape=(jax.ShapeDtypeStruct((EMB, QUART), BF), jax.ShapeDtypeStruct((8, EMB, HALF), BF)),
        in_specs=[any_spec, any_spec, any_spec],
        out_specs=(vmem, vmem),
        scratch_shapes=[
            pltpu.VMEM((NBLK, USERS, CH), F8),
            pltpu.VMEM((RING, PIECE, CH), jnp.int32),
            pltpu.VMEM((3, NBLK, EMB, CH), BF),
            pltpu.VMEM((2, EMB, CH), F32), pltpu.VMEM((2, EMB, CH), F32),
            pltpu.VMEM((4, EMB, CH), F32), pltpu.VMEM((4, EMB, CH), F32),
            pltpu.VMEM((4, EMB, CH), F32), pltpu.VMEM((8, EMB, CH), F32),
            pltpu.VMEM((2, EMB, HALF), F32), pltpu.VMEM((3, EMB, HALF), F32),
            pltpu.VMEM((3, 2, EMB, HALF), BF), pltpu.VMEM((3, EMB, USERS), BF),
            pltpu.VMEM((NBLK, 1, CH), F32), pltpu.VMEM((3, NBLK, 1, CH), F32),
            pltpu.VMEM((NBLK, 8, CH), F32), pltpu.VMEM((8, CH), F32),
            pltpu.VMEM((USERS, 128), F32), pltpu.VMEM((8, USERS), F32), pltpu.VMEM((8, USERS), F32),
            pltpu.VMEM((2, 8, HALF), F32),
            dma((RING,)), dma((NCH + 1,)),
            dma((3 * NCH,)), dma((3 * NCH,)), dma((3 * NCH,)), dma((3 * NCH,)), dma((3 * NCH,)), dma((3 * NCH,)),
            dma((3, NCH)), dma((3, NCH)), dma((1,)), dma((1,)),
            dma((2,)), dma((2,)), dma((4,)), dma((4,)), dma((4,)), dma((8,)),
            dma((3,)), dma((3,)), dma((3,)), dma((3,)), dma((7,)), dma((7,)),
        ],
        compiler_params=pltpu.CompilerParams(collective_id=0, has_side_effects=True, vmem_limit_bytes=67043328),
        name="propagate",
    )(mask, eu0, ei0)


def _lookup_kernel(ids, tri, items, users, part, out_i, out_u, it, ut, pp, pn):
    c = lax.axis_index("col")
    r = lax.axis_index("row")
    out_i[...] = items[...]
    out_u[...] = users[2 * r + c]
    for i in range(QUART // 512):
        it[i * 512:(i + 1) * 512, :EMB] = items[:, i * 512:(i + 1) * 512].astype(F32).T
    for i in range(8):
        ut[i * HALF:(i + 1) * HALF, :EMB] = users[i].astype(F32).T

    @pl.loop(0, 4096 // 16)
    def _(i):
        for w in range(16):
            t = i * 16 + w
            u = ut[pl.ds(ids[0, t], 1), :]
            pp[pl.ds(t, 1), :] = u * it[pl.ds(ids[1, t] & (QUART - 1), 1), :]
            pn[pl.ds(t, 1), :] = u * it[pl.ds(ids[2, t] & (QUART - 1), 1), :]

    @pl.loop(0, 8)
    def _(i):
        for w in range(4):
            at = i * 4 + w
            rows = pl.ds(pl.multiple_of(at * 128, 128), 128)
            sp = jnp.sum(pp[rows, :].T[:EMB], axis=0, keepdims=True)
            sn = jnp.sum(pn[rows, :].T[:EMB], axis=0, keepdims=True)
            own_p = tri[1:2, rows] // QUART == c * 4 + r
            own_n = tri[2:3, rows] // QUART == c * 4 + r
            part[pl.ds(at, 1), :] = jnp.where(own_p, sp, 0.0) - jnp.where(own_n, sn, 0.0)


def _lookup(tri, items, users):
    vmem = pl.BlockSpec(memory_space=pltpu.VMEM)
    smem = pl.BlockSpec(memory_space=pltpu.SMEM)
    return pl.pallas_call(
        _lookup_kernel,
        out_shape=(jax.ShapeDtypeStruct((32, 128), F32), jax.ShapeDtypeStruct((EMB, QUART), BF),
                   jax.ShapeDtypeStruct((EMB, HALF), BF)),
        in_specs=[smem, vmem, vmem, vmem],
        out_specs=(vmem, vmem, vmem),
        scratch_shapes=[pltpu.VMEM((QUART, 128), F32), pltpu.VMEM((4096, 128), F32),
                        pltpu.VMEM((4096, 128), F32), pltpu.VMEM((4096, 128), F32)],
        name="lookup",
    )(tri, tri, items, users)


def _loss_kernel(part, out, got, s_sem, r_sem):
    c = lax.axis_index("col")
    r = lax.axis_index("row")
    me = 2 * r + c
    barrier = pltpu.get_barrier_semaphore()
    for cc in range(2):
        for rr in range(4):
            pl.semaphore_signal(barrier, inc=1, device_id=(cc, rr), device_id_type=MESH)
    pl.semaphore_wait(barrier, 8)

    def copy(i, slot):
        dr, dc = i // 2, i % 2
        return pltpu.make_async_remote_copy(
            src_ref=part, dst_ref=got.at[slot], send_sem=s_sem.at[i], recv_sem=r_sem.at[i],
            device_id=((c + dc) % 2, (r + dr) % 4), device_id_type=MESH)

    def sender(i):
        return 2 * ((r + 4 - i // 2) % 4) + (c + i % 2) % 2

    for i in range(1, 8):
        copy(i, me).start()
    got[me] = part[...]
    for i in range(1, 8):
        copy(i, sender(i)).wait()
    m = got[0]
    for i in range(1, 8):
        m = m + got[i]
    out[...] = jnp.maximum(-m, 0.0) + jnp.log1p(jnp.exp(-jnp.abs(m)))


def _loss(part):
    vmem = pl.BlockSpec(memory_space=pltpu.VMEM)
    return pl.pallas_call(
        _loss_kernel,
        out_shape=jax.ShapeDtypeStruct((32, 128), F32),
        in_specs=[vmem],
        out_specs=vmem,
        scratch_shapes=[pltpu.VMEM((8, 32, 128), F32), pltpu.SemaphoreType.DMA((8,)), pltpu.SemaphoreType.DMA((8,))],
        compiler_params=pltpu.CompilerParams(collective_id=1, has_side_effects=True),
        name="loss",
    )(part)


def solution(mesh):
    def device_body(mask_blk, user_shard, item_shard, triples):
        out_it, users = _main(mask_blk, user_shard.T, item_shard.T)
        part, out_it, out_ut = _lookup(triples.T, out_it, users)
        bpr_loss = _loss(part).reshape(4096)
        return out_ut.T, out_it.T, bpr_loss

    return jax.shard_map(
        device_body,
        mesh=mesh,
        in_specs=(P("row", "col"), P(("row", "col"), None), P(("col", "row"), None), P()),
        out_specs=(P(("row", "col"), None), P(("col", "row"), None), P()),
        check_vma=False,
    )
```

```python
import jax
import jax.numpy as jnp
from jax import lax
from jax.experimental import pallas as pl
from jax.experimental.pallas import tpu as pltpu
from jax.sharding import PartitionSpec as P

LAYERS = 3
F8 = jnp.float8_e4m3fn
BF = jnp.bfloat16
F32 = jnp.float32
MESH = pl.DeviceIdType.MESH

EMB = 64
USERS = 1024
HALF = 512
QUART = 8192
CH = 1024
NCH = 8
NBLK = 32
PIECE = 256
RING = 7
UP_U, DN_U = 256.0, 1.0 / 256.0
UP_I, DN_I = 64.0, 1.0 / 64.0
LAG_B, LAG_C, LAG_D = 2, 3, 4
AHEAD = 3


def _scale(val, s8):
    rows, cols = val.shape
    return (val.reshape(rows // 8, 8, cols) * s8[None]).reshape(rows, cols)


def _main_kernel(mask, eu0, ei0, tri, out_i, ua, ids,
                 m8, stage, pan, snd_a, rcv_a, snd_b, rcv_b, xs, xr,
                 uacc, yr, raw, eus, cs, csr, sib, cacc, rs, rsum, rsum_r, su,
                 st_sem, ld_sem, agx_s, agx_r, agd_s, agd_r, agf_s, agf_r, cs_s, cs_r,
                 rs_s, rs_r, a_s, a_r, b_s, b_r, x_s, x_r, y_s, y_r, w_s, w_r, g_s, g_r):
    c = lax.axis_index("col")
    r = lax.axis_index("row")
    x = r // 2
    k = r % 2
    r_par = 2 * x + (1 - k)
    r_xp = 2 * (1 - x) + k
    r_xq = 2 * (1 - x) + (1 - k)
    par = (c, r_par)
    xpe = (c, r_xp)
    xpa = (c, r_xq)
    ype = (1 - c, r)

    def rcopy(src, dst, ss, rsm, dev):
        return pltpu.make_async_remote_copy(src_ref=src, dst_ref=dst, send_sem=ss, recv_sem=rsm,
                                            device_id=dev, device_id_type=MESH)

    def piece(p):
        blk = p // 4
        row = pl.multiple_of((p % 4) * PIECE, PIECE)
        col = pl.multiple_of((blk % 4) * QUART + (blk // 4) * CH, CH)
        return pltpu.make_async_copy(mask.at[pl.ds(row, PIECE), pl.ds(col, CH)],
                                     stage.at[p % RING], st_sem.at[p % RING])

    for p in range(RING):
        piece(p).start()

    def own_load(j):
        return pltpu.make_async_copy(ei0.at[:, pl.ds(pl.multiple_of(j * CH, CH), CH)],
                                     pan.at[0, j * 4 + r], ld_sem.at[j])

    user_load = pltpu.make_async_copy(eu0, raw.at[0, c], ld_sem.at[NCH])
    for j in range(NCH):
        own_load(j).start()
    user_load.start()

    barrier = pltpu.get_barrier_semaphore()
    for cc in range(2):
        for rr in range(4):
            pl.semaphore_signal(barrier, inc=1, device_id=(cc, rr), device_id_type=MESH)
    pl.semaphore_wait(barrier, 8)

    def ag_x(a, j, q):
        i = a * NCH + j
        ref = pan.at[a, j * 4 + q]
        return rcopy(ref, ref, agx_s.at[i], agx_r.at[i], xpe)

    def ag_d(a, j, q):
        i = a * NCH + j
        ref = pan.at[a, j * 4 + q]
        return rcopy(ref, ref, agd_s.at[i], agd_r.at[i], par)

    def ag_f(a, j, q):
        i = a * NCH + j
        ref = pan.at[a, j * 4 + q]
        return rcopy(ref, ref, agf_s.at[i], agf_r.at[i], par)

    for j in range(NCH):
        own_load(j).wait()
        if j < AHEAD:
            ag_x(0, j, r).start()
        ag_d(0, j, r).start()
    user_load.wait()
    w0 = rcopy(raw.at[0, c], raw.at[0, c], w_s.at[0], w_r.at[0], ype)
    w0.start()

    rs[...] = jnp.zeros_like(rs)
    uacc[...] = jnp.zeros_like(uacc)

    def cs_copy(rel, g, dev):
        return rcopy(cs.at[pl.ds(g * 4, 4)], csr.at[rel, pl.ds(g * 4, 4)], cs_s.at[rel, g], cs_r.at[rel, g], dev)

    def user_prod(a, b):
        es = _scale(pan[a, b].astype(F32), sib[b] * DN_U).astype(BF)
        got = lax.dot_general(es, m8[b], (((1,), (1,)), ((), ())), preferred_element_type=F32)
        uacc[0] += got[:, :HALF]
        uacc[1] += got[:, HALF:]

    def first_users(g):
        for rel, dev in ((0, par), (1, xpe), (2, xpa)):
            cs_copy(rel, g, dev).wait_recv()
        ag_d(0, g, r_par).wait_recv()
        ag_f(0, g, r_xq).wait_recv()

        @pl.loop(0, 4)
        def _(q):
            b = g * 4 + q
            deg = cs[b] + csr[0, b] + csr[1, b] + csr[2, b]
            sib[b] = jnp.broadcast_to(lax.rsqrt(jnp.maximum(deg, 1.0)), (8, CH))
            user_prod(0, b)

    cp_deg = rcopy(rsum, rsum_r, rs_s.at[0], rs_r.at[0], ype)

    @pl.loop(0, NCH)
    def _(g):
        @pl.loop(0, 4)
        def _(q):
            b = g * 4 + q
            cacc[...] = jnp.zeros_like(cacc)

            @pl.loop(0, 4)
            def _(s):
                p = b * 4 + s
                piece(p).wait()
                slot = p % RING

                @pl.loop(0, PIECE // 32)
                def _(i):
                    rows = pl.ds(pl.multiple_of(i * 32, 32), 32)
                    dst = pl.ds(pl.multiple_of(s * PIECE + i * 32, 32), 32)
                    f = stage[slot, rows, :].astype(F32)
                    m8[b, dst, :] = f.astype(F8)
                    cacc[...] += jnp.sum(f.reshape(4, 8, CH), axis=0)
                    part = f[:, :128]
                    for w in range(1, CH // 128):
                        part = part + f[:, w * 128:(w + 1) * 128]
                    rs[dst, :] += part

                @pl.when(p + RING < 4 * NBLK)
                def _():
                    piece(p + RING).start()

            cs[b] = jnp.sum(cacc[...], axis=0, keepdims=True)

        for rel, dev in ((0, par), (1, xpe), (2, xpa)):
            cs_copy(rel, g, dev).start()

        @pl.when(g + AHEAD < NCH)
        def _():
            ag_x(0, g + AHEAD, r).start()

        @pl.when(g == NCH - 1)
        def _():
            rsum[...] = lax.dot_general(jnp.ones((8, 128), BF), rs[...].astype(BF), (((1,), (1,)), ((), ())),
                                        preferred_element_type=F32)
            cp_deg.start()

        ag_x(0, g, r_xp).wait_recv()
        ag_f(0, g, r_xp).start()

        @pl.when((g >= 1) & (g < NCH - 1))
        def _():
            first_users(g - 1)

    cp_deg.wait()
    w0.wait()
    deg_u = lax.rsqrt(jnp.maximum(rsum[...] + rsum_r[...], 1.0))
    su[0] = deg_u[:, :HALF]
    su[1] = deg_u[:, HALF:]

    def user_operand(lay):
        for h in range(2):
            eus[lay, :, h * HALF:(h + 1) * HALF] = _scale(raw[lay, h].astype(F32), su[h] * DN_I).astype(BF)

    user_operand(0)

    def prod(lay, b):
        return jnp.dot(eus[lay], m8[b], preferred_element_type=F32)

    def cp_a(g):
        return rcopy(snd_a.at[g % 2], rcv_a.at[g % 2], a_s.at[g % 2], a_r.at[g % 2], par)

    def cp_b(g):
        return rcopy(snd_b.at[g % 4], rcv_b.at[g % 4], b_s.at[g % 4], b_r.at[g % 4], par)

    def cp_x(g):
        return rcopy(xs.at[g % 4], xr.at[g % 8], x_s.at[g % 4], x_r.at[g % 8], xpe)

    def step_a(g):
        lay = g // NCH
        b = (g % NCH) * 4

        @pl.when(g >= 2)
        def _():
            cp_a(g - 2).wait_send()

        snd_a[g % 2] = prod(lay, b + r_xq)
        cp_a(g).start()

        @pl.when(g >= 4)
        def _():
            cp_x(g - 4).wait_send()

        xs[g % 4] = prod(lay, b + r_xp)
        cp_a(g).wait_recv()
        xs[g % 4] += rcv_a[g % 2]
        cp_x(g).start()

        @pl.when(g >= 4)
        def _():
            cp_b(g - 4).wait_send()

        snd_b[g % 4] = prod(lay, b + r_par)
        cp_b(g).start()

    def step_b(g):
        lay = g // NCH
        j = g % NCH
        b = j * 4 + r
        own = prod(lay, b)
        cp_b(g).wait_recv()
        own = own + rcv_b[g % 4]
        cp_x(g).wait_recv()
        emb = _scale(own + xr[g % 8], sib[b] * UP_I).astype(BF)

        @pl.when(lay < 2)
        def _():
            pan[lay + 1, b] = emb
            ag_x(lay + 1, j, r).start()
            ag_d(lay + 1, j, r).start()

        @pl.when(lay == 2)
        def _():
            tot = pan[0, b].astype(F32) + pan[1, b].astype(F32) + pan[2, b].astype(F32) + emb.astype(F32)
            out_i[:, pl.ds(pl.multiple_of(j * CH, CH), CH)] = (tot * 0.25).astype(BF)

    def step_c(g):
        a = g // NCH + 1
        ag_x(a, g % NCH, r_xp).wait_recv()
        ag_f(a, g % NCH, r_xp).start()

    def step_d(g):
        a = g // NCH + 1
        j = g % NCH
        ag_d(a, j, r_par).wait_recv()
        ag_f(a, j, r_xq).wait_recv()

        @pl.loop(0, 4)
        def _(q):
            user_prod(a, j * 4 + q)

    def cp_y(lay):
        return rcopy(uacc.at[1 - c], yr.at[lay - 1], y_s.at[lay - 1], y_r.at[lay - 1], ype)

    def cp_w(lay):
        return rcopy(raw.at[lay, c], raw.at[lay, c], w_s.at[lay], w_r.at[lay], ype)

    def user_emb(lay):
        cp_y(lay).wait()
        emb = _scale(uacc[c] + yr[lay - 1], su[c] * UP_U).astype(BF)
        uacc[...] = jnp.zeros_like(uacc)
        return emb

    def finish_user(lay):
        raw[lay, c] = user_emb(lay)
        cp_w(lay).start()

    def load_user(lay):
        cp_w(lay).wait()
        user_operand(lay)

    def cp_g(i, blk, dev):
        return rcopy(ua.at[blk], ua.at[blk], g_s.at[i], g_r.at[i], dev)

    own_u = 2 * r + c
    D1, D2 = NCH - 1 + LAG_D, 2 * NCH - 1 + LAG_D

    @pl.loop(0, LAYERS * NCH + LAG_B)
    def _(t):
        @pl.when(t < LAYERS * NCH)
        def _():
            step_a(t)

        @pl.when(t < 2)
        def _():
            first_users(NCH - 2 + t)

        @pl.when(t == 1)
        def _():
            cp_y(1).start()

        @pl.when(t == 2)
        def _():
            finish_user(1)
            for i in range(32):
                for w in range(3):
                    ids[w, i:i + 1, :] = tri[w:w + 1, i * 128:(i + 1) * 128] & ((4096 if w == 0 else QUART) - 1)

        @pl.when(t == 3)
        def _():
            load_user(1)

        @pl.when(t == D1 + 1)
        def _():
            finish_user(2)

        @pl.when(t == D1 + 2)
        def _():
            load_user(2)

        @pl.when(t == D2 + 1)
        def _():
            emb = user_emb(3).astype(F32)
            tot = raw[0, c].astype(F32) + raw[1, c].astype(F32) + raw[2, c].astype(F32) + emb
            ua[own_u] = (tot * 0.25).astype(BF)
            cp_g(0, own_u, ype).start()
            cp_g(1, own_u, par).start()
            cp_g(2, own_u, xpe).start()

        @pl.when(t == D2 + 2)
        def _():
            cp_g(0, 2 * r + 1 - c, ype).wait_recv()
            cp_g(1, 2 * r_par + c, par).wait_recv()
            cp_g(2, 2 * r_xp + c, xpe).wait_recv()
            cp_g(3, 2 * r + 1 - c, par).start()
            cp_g(4, 2 * r_xp + c, par).start()
            cp_g(5, 2 * r_xp + c, ype).start()

        @pl.when(t == D2 + 3)
        def _():
            cp_g(3, 2 * r_par + 1 - c, par).wait_recv()
            cp_g(4, 2 * r_xq + c, par).wait_recv()
            cp_g(5, 2 * r_xp + 1 - c, ype).wait_recv()
            cp_g(6, 2 * r_xp + 1 - c, par).start()

        @pl.when(t == D2 + 4)
        def _():
            cp_g(6, 2 * r_xq + 1 - c, par).wait_recv()

        @pl.when(t >= LAG_B)
        def _():
            step_b(t - LAG_B)

        @pl.when((t >= LAG_C) & (t < 2 * NCH + LAG_C))
        def _():
            step_c(t - LAG_C)

        @pl.when((t >= LAG_D) & (t < 2 * NCH + LAG_D))
        def _():
            step_d(t - LAG_D)

        @pl.when(t == D1)
        def _():
            cp_y(2).start()

        @pl.when(t == D2)
        def _():
            cp_y(3).start()

    last = LAYERS * NCH
    for g in range(last - 2, last):
        cp_a(g).wait_send()
    for g in range(last - 4, last):
        cp_b(g).wait_send()
    for g in range(last - 4, last):
        cp_x(g).wait_send()
    for i in range(7):
        cp_g(i, own_u, par).wait_send()

    @pl.loop(0, NCH)
    def _(j):
        for rel, dev in ((0, par), (1, xpe), (2, xpa)):
            cs_copy(rel, j, dev).wait_send()

    @pl.loop(0, 3 * NCH)
    def _(i):
        ag_x(i // NCH, i % NCH, r).wait_send()
        ag_d(i // NCH, i % NCH, r).wait_send()
        ag_f(i // NCH, i % NCH, r_xp).wait_send()


def _main(mask, eu0, ei0, tri):
    dma = pltpu.SemaphoreType.DMA
    any_spec = pl.BlockSpec(memory_space=pl.ANY)
    vmem = pl.BlockSpec(memory_space=pltpu.VMEM)
    return pl.pallas_call(
        _main_kernel,
        out_shape=(jax.ShapeDtypeStruct((EMB, QUART), BF), jax.ShapeDtypeStruct((8, EMB, HALF), BF),
                   jax.ShapeDtypeStruct((3, 32, 128), jnp.int32)),
        in_specs=[any_spec, any_spec, any_spec, vmem],
        out_specs=(vmem, vmem, vmem),
        scratch_shapes=[
            pltpu.VMEM((NBLK, USERS, CH), F8),
            pltpu.VMEM((RING, PIECE, CH), jnp.int32),
            pltpu.VMEM((3, NBLK, EMB, CH), BF),
            pltpu.VMEM((2, EMB, CH), F32), pltpu.VMEM((2, EMB, CH), F32),
            pltpu.VMEM((4, EMB, CH), F32), pltpu.VMEM((4, EMB, CH), F32),
            pltpu.VMEM((4, EMB, CH), F32), pltpu.VMEM((8, EMB, CH), F32),
            pltpu.VMEM((2, EMB, HALF), F32), pltpu.VMEM((3, EMB, HALF), F32),
            pltpu.VMEM((3, 2, EMB, HALF), BF), pltpu.VMEM((3, EMB, USERS), BF),
            pltpu.VMEM((NBLK, 1, CH), F32), pltpu.VMEM((3, NBLK, 1, CH), F32),
            pltpu.VMEM((NBLK, 8, CH), F32), pltpu.VMEM((8, CH), F32),
            pltpu.VMEM((USERS, 128), F32), pltpu.VMEM((8, USERS), F32), pltpu.VMEM((8, USERS), F32),
            pltpu.VMEM((2, 8, HALF), F32),
            dma((RING,)), dma((NCH + 1,)),
            dma((3 * NCH,)), dma((3 * NCH,)), dma((3 * NCH,)), dma((3 * NCH,)), dma((3 * NCH,)), dma((3 * NCH,)),
            dma((3, NCH)), dma((3, NCH)), dma((1,)), dma((1,)),
            dma((2,)), dma((2,)), dma((4,)), dma((4,)), dma((4,)), dma((8,)),
            dma((3,)), dma((3,)), dma((3,)), dma((3,)), dma((7,)), dma((7,)),
        ],
        compiler_params=pltpu.CompilerParams(collective_id=0, has_side_effects=True, vmem_limit_bytes=67043328),
        name="propagate",
    )(mask, eu0, ei0, tri)


def _lookup_kernel(uid, pid, nid, tri, items, users, part, out_i, out_u, it, ut, pp, pn):
    c = lax.axis_index("col")
    r = lax.axis_index("row")
    out_i[...] = items[...]
    out_u[...] = users[2 * r + c]
    for i in range(QUART // 512):
        it[i * 512:(i + 1) * 512, :EMB] = items[:, i * 512:(i + 1) * 512].astype(F32).T
    for i in range(8):
        ut[i * HALF:(i + 1) * HALF, :EMB] = users[i].astype(F32).T

    @pl.loop(0, 4096 // 64)
    def _(i):
        for w in range(64):
            t = i * 64 + w
            u = ut[pl.ds(uid[t], 1), :]
            pp[pl.ds(t, 1), :] = u * it[pl.ds(pid[t], 1), :]
            pn[pl.ds(t, 1), :] = u * it[pl.ds(nid[t], 1), :]

    @pl.loop(0, 8)
    def _(i):
        for w in range(4):
            at = i * 4 + w
            rows = pl.ds(pl.multiple_of(at * 128, 128), 128)
            sp = jnp.sum(pp[rows, :].T[:EMB], axis=0, keepdims=True)
            sn = jnp.sum(pn[rows, :].T[:EMB], axis=0, keepdims=True)
            own_p = tri[1:2, rows] // QUART == c * 4 + r
            own_n = tri[2:3, rows] // QUART == c * 4 + r
            part[pl.ds(at, 1), :] = jnp.where(own_p, sp, 0.0) - jnp.where(own_n, sn, 0.0)


def _lookup(ids, tri, items, users):
    vmem = pl.BlockSpec(memory_space=pltpu.VMEM)
    smem = pl.BlockSpec(memory_space=pltpu.SMEM)
    return pl.pallas_call(
        _lookup_kernel,
        out_shape=(jax.ShapeDtypeStruct((32, 128), F32), jax.ShapeDtypeStruct((EMB, QUART), BF),
                   jax.ShapeDtypeStruct((EMB, HALF), BF)),
        in_specs=[smem, smem, smem, vmem, vmem, vmem],
        out_specs=(vmem, vmem, vmem),
        scratch_shapes=[pltpu.VMEM((QUART, 128), F32), pltpu.VMEM((4096, 128), F32),
                        pltpu.VMEM((4096, 128), F32), pltpu.VMEM((4096, 128), F32)],
        name="lookup",
    )(ids[0].reshape(4096), ids[1].reshape(4096), ids[2].reshape(4096), tri, items, users)


def _loss_kernel(part, out, got, s_sem, r_sem):
    c = lax.axis_index("col")
    r = lax.axis_index("row")
    me = 2 * r + c
    barrier = pltpu.get_barrier_semaphore()
    for cc in range(2):
        for rr in range(4):
            pl.semaphore_signal(barrier, inc=1, device_id=(cc, rr), device_id_type=MESH)
    pl.semaphore_wait(barrier, 8)

    def copy(i, slot):
        dr, dc = i // 2, i % 2
        return pltpu.make_async_remote_copy(
            src_ref=part, dst_ref=got.at[slot], send_sem=s_sem.at[i], recv_sem=r_sem.at[i],
            device_id=((c + dc) % 2, (r + dr) % 4), device_id_type=MESH)

    def sender(i):
        return 2 * ((r + 4 - i // 2) % 4) + (c + i % 2) % 2

    for i in range(1, 8):
        copy(i, me).start()
    got[me] = part[...]
    for i in range(1, 8):
        copy(i, sender(i)).wait()
    m = got[0]
    for i in range(1, 8):
        m = m + got[i]
    out[...] = jnp.maximum(-m, 0.0) + jnp.log1p(jnp.exp(-jnp.abs(m)))


def _loss(part):
    vmem = pl.BlockSpec(memory_space=pltpu.VMEM)
    return pl.pallas_call(
        _loss_kernel,
        out_shape=jax.ShapeDtypeStruct((32, 128), F32),
        in_specs=[vmem],
        out_specs=vmem,
        scratch_shapes=[pltpu.VMEM((8, 32, 128), F32), pltpu.SemaphoreType.DMA((8,)), pltpu.SemaphoreType.DMA((8,))],
        compiler_params=pltpu.CompilerParams(collective_id=1, has_side_effects=True),
        name="loss",
    )(part)


def solution(mesh):
    def device_body(mask_blk, user_shard, item_shard, triples):
        tri = triples.T
        out_it, users, ids = _main(mask_blk, user_shard.T, item_shard.T, tri)
        part, out_it, out_ut = _lookup(ids, tri, out_it, users)
        bpr_loss = _loss(part).reshape(4096)
        return out_ut.T, out_it.T, bpr_loss

    return jax.shard_map(
        device_body,
        mesh=mesh,
        in_specs=(P("row", "col"), P(("row", "col"), None), P(("col", "row"), None), P()),
        out_specs=(P(("row", "col"), None), P(("col", "row"), None), P()),
        check_vma=False,
    )
```

```python
import jax
import jax.numpy as jnp
from jax import lax
from jax.experimental import pallas as pl
from jax.experimental.pallas import tpu as pltpu
from jax.sharding import PartitionSpec as P

LAYERS = 3
F8 = jnp.float8_e4m3fn
BF = jnp.bfloat16
F32 = jnp.float32
MESH = pl.DeviceIdType.MESH

EMB = 64
USERS = 1024
HALF = 512
QUART = 8192
CH = 1024
NCH = 8
NBLK = 32
PIECE = 256
STEP = 64
RING = 7
UP_U, DN_U = 256.0, 1.0 / 256.0
UP_I, DN_I = 64.0, 1.0 / 64.0
LAG_B, LAG_C, LAG_D = 2, 3, 4
AHEAD = 3


def _scale(val, s8):
    rows, cols = val.shape
    return (val.reshape(rows // 8, 8, cols) * s8[None]).reshape(rows, cols)


def _main_kernel(mask, eu0, ei0, tri, out_i, ua, ids,
                 m8, stage, pan, snd_a, rcv_a, snd_b, rcv_b, xs, xr,
                 uacc, yr, raw, eus, cs, csr, sib, cacc, rs, rsum, rsum_r, su,
                 st_sem, ld_sem, agx_s, agx_r, agd_s, agd_r, agf_s, agf_r, cs_s, cs_r,
                 rs_s, rs_r, a_s, a_r, b_s, b_r, x_s, x_r, y_s, y_r, w_s, w_r, g_s, g_r):
    c = lax.axis_index("col")
    r = lax.axis_index("row")
    x = r // 2
    k = r % 2
    r_par = 2 * x + (1 - k)
    r_xp = 2 * (1 - x) + k
    r_xq = 2 * (1 - x) + (1 - k)
    par = (c, r_par)
    xpe = (c, r_xp)
    xpa = (c, r_xq)
    ype = (1 - c, r)

    def rcopy(src, dst, ss, rsm, dev):
        return pltpu.make_async_remote_copy(src_ref=src, dst_ref=dst, send_sem=ss, recv_sem=rsm,
                                            device_id=dev, device_id_type=MESH)

    def piece(p):
        blk = p // 4
        row = pl.multiple_of((p % 4) * PIECE, PIECE)
        col = pl.multiple_of((blk % 4) * QUART + (blk // 4) * CH, CH)
        return pltpu.make_async_copy(mask.at[pl.ds(row, PIECE), pl.ds(col, CH)],
                                     stage.at[p % RING], st_sem.at[p % RING])

    def own_load(j):
        return pltpu.make_async_copy(ei0.at[:, pl.ds(pl.multiple_of(j * CH, CH), CH)],
                                     pan.at[0, j * 4 + r], ld_sem.at[j])

    user_load = pltpu.make_async_copy(eu0, raw.at[0, c], ld_sem.at[NCH])
    for j in range(NCH):
        own_load(j).start()
    user_load.start()
    for p in range(RING):
        piece(p).start()

    barrier = pltpu.get_barrier_semaphore()
    for cc in range(2):
        for rr in range(4):
            pl.semaphore_signal(barrier, inc=1, device_id=(cc, rr), device_id_type=MESH)
    pl.semaphore_wait(barrier, 8)

    def ag_x(a, j, q):
        i = a * NCH + j
        ref = pan.at[a, j * 4 + q]
        return rcopy(ref, ref, agx_s.at[i], agx_r.at[i], xpe)

    def ag_d(a, j, q):
        i = a * NCH + j
        ref = pan.at[a, j * 4 + q]
        return rcopy(ref, ref, agd_s.at[i], agd_r.at[i], par)

    def ag_f(a, j, q):
        i = a * NCH + j
        ref = pan.at[a, j * 4 + q]
        return rcopy(ref, ref, agf_s.at[i], agf_r.at[i], par)

    for j in range(NCH):
        own_load(j).wait()
        if j < AHEAD:
            ag_x(0, j, r).start()
        ag_d(0, j, r).start()
    user_load.wait()
    w0 = rcopy(raw.at[0, c], raw.at[0, c], w_s.at[0], w_r.at[0], ype)
    w0.start()

    rs[...] = jnp.zeros_like(rs)
    uacc[...] = jnp.zeros_like(uacc)

    def cs_copy(rel, g, dev):
        return rcopy(cs.at[pl.ds(g * 4, 4)], csr.at[rel, pl.ds(g * 4, 4)], cs_s.at[rel, g], cs_r.at[rel, g], dev)

    def user_prod(a, b):
        es = _scale(pan[a, b].astype(F32), sib[b] * DN_U).astype(BF)
        got = lax.dot_general(es, m8[b], (((1,), (1,)), ((), ())), preferred_element_type=F32)
        uacc[0] += got[:, :HALF]
        uacc[1] += got[:, HALF:]

    def first_users(g):
        for rel, dev in ((0, par), (1, xpe), (2, xpa)):
            cs_copy(rel, g, dev).wait_recv()
        ag_d(0, g, r_par).wait_recv()
        ag_f(0, g, r_xq).wait_recv()

        @pl.loop(0, 4)
        def _(q):
            b = g * 4 + q
            deg = cs[b] + csr[0, b] + csr[1, b] + csr[2, b]
            sib[b] = jnp.broadcast_to(lax.rsqrt(jnp.maximum(deg, 1.0)), (8, CH))
            user_prod(0, b)

    cp_deg = rcopy(rsum, rsum_r, rs_s.at[0], rs_r.at[0], ype)

    @pl.loop(0, NCH)
    def _(g):
        @pl.loop(0, 4)
        def _(q):
            b = g * 4 + q
            cacc[...] = jnp.zeros_like(cacc)

            @pl.loop(0, 4)
            def _(s):
                p = b * 4 + s
                piece(p).wait()
                slot = p % RING

                @pl.loop(0, PIECE // STEP)
                def _(i):
                    rows = pl.ds(pl.multiple_of(i * STEP, STEP), STEP)
                    dst = pl.ds(pl.multiple_of(s * PIECE + i * STEP, STEP), STEP)
                    f = stage[slot, rows, :].astype(F32)
                    m8[b, dst, :] = f.astype(F8)
                    cacc[...] += jnp.sum(f.reshape(STEP // 8, 8, CH), axis=0)
                    part = f[:, :128]
                    for w in range(1, CH // 128):
                        part = part + f[:, w * 128:(w + 1) * 128]
                    rs[dst, :] += part

                @pl.when(p + RING < 4 * NBLK)
                def _():
                    piece(p + RING).start()

            cs[b] = jnp.sum(cacc[...], axis=0, keepdims=True)

        for rel, dev in ((0, par), (1, xpe), (2, xpa)):
            cs_copy(rel, g, dev).start()

        @pl.when(g + AHEAD < NCH)
        def _():
            ag_x(0, g + AHEAD, r).start()

        @pl.when(g == NCH - 1)
        def _():
            rsum[...] = lax.dot_general(jnp.ones((8, 128), BF), rs[...].astype(BF), (((1,), (1,)), ((), ())),
                                        preferred_element_type=F32)
            cp_deg.start()

        ag_x(0, g, r_xp).wait_recv()
        ag_f(0, g, r_xp).start()

    cp_deg.wait()
    w0.wait()
    deg_u = lax.rsqrt(jnp.maximum(rsum[...] + rsum_r[...], 1.0))
    su[0] = deg_u[:, :HALF]
    su[1] = deg_u[:, HALF:]

    def user_operand(lay):
        for h in range(2):
            eus[lay, :, h * HALF:(h + 1) * HALF] = _scale(raw[lay, h].astype(F32), su[h] * DN_I).astype(BF)

    user_operand(0)

    def prod(lay, b):
        return jnp.dot(eus[lay], m8[b], preferred_element_type=F32)

    def cp_a(g):
        return rcopy(snd_a.at[g % 2], rcv_a.at[g % 2], a_s.at[g % 2], a_r.at[g % 2], par)

    def cp_b(g):
        return rcopy(snd_b.at[g % 4], rcv_b.at[g % 4], b_s.at[g % 4], b_r.at[g % 4], par)

    def cp_x(g):
        return rcopy(xs.at[g % 4], xr.at[g % 8], x_s.at[g % 4], x_r.at[g % 8], xpe)

    def step_a(g):
        lay = g // NCH
        b = (g % NCH) * 4

        @pl.when(g >= 2)
        def _():
            cp_a(g - 2).wait_send()

        snd_a[g % 2] = prod(lay, b + r_xq)
        cp_a(g).start()

        @pl.when(g >= 4)
        def _():
            cp_x(g - 4).wait_send()

        xs[g % 4] = prod(lay, b + r_xp)
        cp_a(g).wait_recv()
        xs[g % 4] += rcv_a[g % 2]
        cp_x(g).start()

        @pl.when(g >= 4)
        def _():
            cp_b(g - 4).wait_send()

        snd_b[g % 4] = prod(lay, b + r_par)
        cp_b(g).start()

    def step_b(g):
        lay = g // NCH
        j = g % NCH
        b = j * 4 + r
        own = prod(lay, b)
        cp_b(g).wait_recv()
        own = own + rcv_b[g % 4]
        cp_x(g).wait_recv()
        emb = _scale(own + xr[g % 8], sib[b] * UP_I).astype(BF)

        @pl.when(lay < 2)
        def _():
            pan[lay + 1, b] = emb
            ag_x(lay + 1, j, r).start()
            ag_d(lay + 1, j, r).start()

        @pl.when(lay == 2)
        def _():
            tot = pan[0, b].astype(F32) + pan[1, b].astype(F32) + pan[2, b].astype(F32) + emb.astype(F32)
            out_i[:, pl.ds(pl.multiple_of(j * CH, CH), CH)] = (tot * 0.25).astype(BF)

    def step_c(g):
        a = g // NCH + 1
        ag_x(a, g % NCH, r_xp).wait_recv()
        ag_f(a, g % NCH, r_xp).start()

    def step_d(g):
        a = g // NCH + 1
        j = g % NCH
        ag_d(a, j, r_par).wait_recv()
        ag_f(a, j, r_xq).wait_recv()

        @pl.loop(0, 4)
        def _(q):
            user_prod(a, j * 4 + q)

    def cp_y(lay):
        return rcopy(uacc.at[1 - c], yr.at[lay - 1], y_s.at[lay - 1], y_r.at[lay - 1], ype)

    def cp_w(lay):
        return rcopy(raw.at[lay, c], raw.at[lay, c], w_s.at[lay], w_r.at[lay], ype)

    def user_emb(lay):
        cp_y(lay).wait()
        emb = _scale(uacc[c] + yr[lay - 1], su[c] * UP_U).astype(BF)
        uacc[...] = jnp.zeros_like(uacc)
        return emb

    def finish_user(lay):
        raw[lay, c] = user_emb(lay)
        cp_w(lay).start()

    def load_user(lay):
        cp_w(lay).wait()
        user_operand(lay)

    def cp_g(i, blk, dev):
        return rcopy(ua.at[blk], ua.at[blk], g_s.at[i], g_r.at[i], dev)

    own_u = 2 * r + c
    D1, D2 = NCH - 1 + LAG_D, 2 * NCH - 1 + LAG_D

    @pl.loop(0, LAYERS * NCH + LAG_B)
    def _(t):
        @pl.when(t < LAYERS * NCH)
        def _():
            step_a(t)

        @pl.when(t < 4)
        def _():
            first_users(2 * t)
            first_users(2 * t + 1)

        @pl.when(t == 3)
        def _():
            cp_y(1).start()

        @pl.when(t == 4)
        def _():
            finish_user(1)
            for i in range(32):
                for w in range(3):
                    ids[w, i:i + 1, :] = tri[w:w + 1, i * 128:(i + 1) * 128] & ((4096 if w == 0 else QUART) - 1)

        @pl.when(t == 5)
        def _():
            load_user(1)

        @pl.when(t == D1 + 1)
        def _():
            finish_user(2)

        @pl.when(t == D1 + 2)
        def _():
            load_user(2)

        @pl.when(t == D2 + 1)
        def _():
            emb = user_emb(3).astype(F32)
            tot = raw[0, c].astype(F32) + raw[1, c].astype(F32) + raw[2, c].astype(F32) + emb
            ua[own_u] = (tot * 0.25).astype(BF)
            cp_g(0, own_u, ype).start()
            cp_g(1, own_u, par).start()
            cp_g(2, own_u, xpe).start()

        @pl.when(t == D2 + 2)
        def _():
            cp_g(0, 2 * r + 1 - c, ype).wait_recv()
            cp_g(1, 2 * r_par + c, par).wait_recv()
            cp_g(2, 2 * r_xp + c, xpe).wait_recv()
            cp_g(3, 2 * r + 1 - c, par).start()
            cp_g(4, 2 * r_xp + c, par).start()
            cp_g(5, 2 * r_xp + c, ype).start()

        @pl.when(t == D2 + 3)
        def _():
            cp_g(3, 2 * r_par + 1 - c, par).wait_recv()
            cp_g(4, 2 * r_xq + c, par).wait_recv()
            cp_g(5, 2 * r_xp + 1 - c, ype).wait_recv()
            cp_g(6, 2 * r_xp + 1 - c, par).start()

        @pl.when(t == D2 + 4)
        def _():
            cp_g(6, 2 * r_xq + 1 - c, par).wait_recv()

        @pl.when(t >= LAG_B)
        def _():
            step_b(t - LAG_B)

        @pl.when((t >= LAG_C) & (t < 2 * NCH + LAG_C))
        def _():
            step_c(t - LAG_C)

        @pl.when((t >= LAG_D) & (t < 2 * NCH + LAG_D))
        def _():
            step_d(t - LAG_D)

        @pl.when(t == D1)
        def _():
            cp_y(2).start()

        @pl.when(t == D2)
        def _():
            cp_y(3).start()

    last = LAYERS * NCH
    for g in range(last - 2, last):
        cp_a(g).wait_send()
    for g in range(last - 4, last):
        cp_b(g).wait_send()
    for g in range(last - 4, last):
        cp_x(g).wait_send()
    for i in range(7):
        cp_g(i, own_u, par).wait_send()

    @pl.loop(0, NCH)
    def _(j):
        for rel, dev in ((0, par), (1, xpe), (2, xpa)):
            cs_copy(rel, j, dev).wait_send()

    @pl.loop(0, 3 * NCH)
    def _(i):
        ag_x(i // NCH, i % NCH, r).wait_send()
        ag_d(i // NCH, i % NCH, r).wait_send()
        ag_f(i // NCH, i % NCH, r_xp).wait_send()


def _main(mask, eu0, ei0, tri):
    dma = pltpu.SemaphoreType.DMA
    any_spec = pl.BlockSpec(memory_space=pl.ANY)
    vmem = pl.BlockSpec(memory_space=pltpu.VMEM)
    return pl.pallas_call(
        _main_kernel,
        out_shape=(jax.ShapeDtypeStruct((EMB, QUART), BF), jax.ShapeDtypeStruct((8, EMB, HALF), BF),
                   jax.ShapeDtypeStruct((3, 32, 128), jnp.int32)),
        in_specs=[any_spec, any_spec, any_spec, vmem],
        out_specs=(vmem, vmem, vmem),
        scratch_shapes=[
            pltpu.VMEM((NBLK, USERS, CH), F8),
            pltpu.VMEM((RING, PIECE, CH), jnp.int32),
            pltpu.VMEM((3, NBLK, EMB, CH), BF),
            pltpu.VMEM((2, EMB, CH), F32), pltpu.VMEM((2, EMB, CH), F32),
            pltpu.VMEM((4, EMB, CH), F32), pltpu.VMEM((4, EMB, CH), F32),
            pltpu.VMEM((4, EMB, CH), F32), pltpu.VMEM((8, EMB, CH), F32),
            pltpu.VMEM((2, EMB, HALF), F32), pltpu.VMEM((3, EMB, HALF), F32),
            pltpu.VMEM((3, 2, EMB, HALF), BF), pltpu.VMEM((3, EMB, USERS), BF),
            pltpu.VMEM((NBLK, 1, CH), F32), pltpu.VMEM((3, NBLK, 1, CH), F32),
            pltpu.VMEM((NBLK, 8, CH), F32), pltpu.VMEM((8, CH), F32),
            pltpu.VMEM((USERS, 128), F32), pltpu.VMEM((8, USERS), F32), pltpu.VMEM((8, USERS), F32),
            pltpu.VMEM((2, 8, HALF), F32),
            dma((RING,)), dma((NCH + 1,)),
            dma((3 * NCH,)), dma((3 * NCH,)), dma((3 * NCH,)), dma((3 * NCH,)), dma((3 * NCH,)), dma((3 * NCH,)),
            dma((3, NCH)), dma((3, NCH)), dma((1,)), dma((1,)),
            dma((2,)), dma((2,)), dma((4,)), dma((4,)), dma((4,)), dma((8,)),
            dma((3,)), dma((3,)), dma((3,)), dma((3,)), dma((7,)), dma((7,)),
        ],
        compiler_params=pltpu.CompilerParams(collective_id=0, has_side_effects=True, vmem_limit_bytes=67043328),
        name="propagate",
    )(mask, eu0, ei0, tri)


def _lookup_kernel(uid, pid, nid, tri, items, users, part, out_i, out_u, it, ut, pp, pn):
    c = lax.axis_index("col")
    r = lax.axis_index("row")
    out_i[...] = items[...]
    out_u[...] = users[2 * r + c]
    for i in range(QUART // 512):
        it[i * 512:(i + 1) * 512, :EMB] = items[:, i * 512:(i + 1) * 512].astype(F32).T
    for i in range(8):
        ut[i * HALF:(i + 1) * HALF, :EMB] = users[i].astype(F32).T

    @pl.loop(0, 4096 // 64)
    def _(i):
        for w in range(64):
            t = i * 64 + w
            u = ut[pl.ds(uid[t], 1), :]
            pp[pl.ds(t, 1), :] = u * it[pl.ds(pid[t], 1), :]
            pn[pl.ds(t, 1), :] = u * it[pl.ds(nid[t], 1), :]

    @pl.loop(0, 8)
    def _(i):
        for w in range(4):
            at = i * 4 + w
            rows = pl.ds(pl.multiple_of(at * 128, 128), 128)
            sp = jnp.sum(pp[rows, :].T[:EMB], axis=0, keepdims=True)
            sn = jnp.sum(pn[rows, :].T[:EMB], axis=0, keepdims=True)
            own_p = tri[1:2, rows] // QUART == c * 4 + r
            own_n = tri[2:3, rows] // QUART == c * 4 + r
            part[pl.ds(at, 1), :] = jnp.where(own_p, sp, 0.0) - jnp.where(own_n, sn, 0.0)


def _lookup(ids, tri, items, users):
    vmem = pl.BlockSpec(memory_space=pltpu.VMEM)
    smem = pl.BlockSpec(memory_space=pltpu.SMEM)
    return pl.pallas_call(
        _lookup_kernel,
        out_shape=(jax.ShapeDtypeStruct((32, 128), F32), jax.ShapeDtypeStruct((EMB, QUART), BF),
                   jax.ShapeDtypeStruct((EMB, HALF), BF)),
        in_specs=[smem, smem, smem, vmem, vmem, vmem],
        out_specs=(vmem, vmem, vmem),
        scratch_shapes=[pltpu.VMEM((QUART, 128), F32), pltpu.VMEM((4096, 128), F32),
                        pltpu.VMEM((4096, 128), F32), pltpu.VMEM((4096, 128), F32)],
        name="lookup",
    )(ids[0].reshape(4096), ids[1].reshape(4096), ids[2].reshape(4096), tri, items, users)


def _loss_kernel(part, out, got, s_sem, r_sem):
    c = lax.axis_index("col")
    r = lax.axis_index("row")
    me = 2 * r + c
    barrier = pltpu.get_barrier_semaphore()
    for cc in range(2):
        for rr in range(4):
            pl.semaphore_signal(barrier, inc=1, device_id=(cc, rr), device_id_type=MESH)
    pl.semaphore_wait(barrier, 8)

    def copy(i, slot):
        dr, dc = i // 2, i % 2
        return pltpu.make_async_remote_copy(
            src_ref=part, dst_ref=got.at[slot], send_sem=s_sem.at[i], recv_sem=r_sem.at[i],
            device_id=((c + dc) % 2, (r + dr) % 4), device_id_type=MESH)

    def sender(i):
        return 2 * ((r + 4 - i // 2) % 4) + (c + i % 2) % 2

    for i in range(1, 8):
        copy(i, me).start()
    got[me] = part[...]
    for i in range(1, 8):
        copy(i, sender(i)).wait()
    m = got[0]
    for i in range(1, 8):
        m = m + got[i]
    out[...] = jnp.maximum(-m, 0.0) + jnp.log1p(jnp.exp(-jnp.abs(m)))


def _loss(part):
    vmem = pl.BlockSpec(memory_space=pltpu.VMEM)
    return pl.pallas_call(
        _loss_kernel,
        out_shape=jax.ShapeDtypeStruct((32, 128), F32),
        in_specs=[vmem],
        out_specs=vmem,
        scratch_shapes=[pltpu.VMEM((8, 32, 128), F32), pltpu.SemaphoreType.DMA((8,)), pltpu.SemaphoreType.DMA((8,))],
        compiler_params=pltpu.CompilerParams(collective_id=1, has_side_effects=True),
        name="loss",
    )(part)


def solution(mesh):
    def device_body(mask_blk, user_shard, item_shard, triples):
        tri = triples.T
        out_it, users, ids = _main(mask_blk, user_shard.T, item_shard.T, tri)
        part, out_it, out_ut = _lookup(ids, tri, out_it, users)
        bpr_loss = _loss(part).reshape(4096)
        return out_ut.T, out_it.T, bpr_loss

    return jax.shard_map(
        device_body,
        mesh=mesh,
        in_specs=(P("row", "col"), P(("row", "col"), None), P(("col", "row"), None), P()),
        out_specs=(P(("row", "col"), None), P(("col", "row"), None), P()),
        check_vma=False,
    )
```

```python
import jax
import jax.numpy as jnp
from jax import lax
from jax.experimental import pallas as pl
from jax.experimental.pallas import tpu as pltpu
from jax.sharding import PartitionSpec as P

LAYERS = 3
F8 = jnp.float8_e4m3fn
BF = jnp.bfloat16
F32 = jnp.float32
MESH = pl.DeviceIdType.MESH

EMB = 64
USERS = 1024
HALF = 512
QUART = 8192
CH = 1024
NCH = 8
NBLK = 32
PIECE = 256
STEP = 64
RING = 7
UP_U, DN_U = 256.0, 1.0 / 256.0
UP_I, DN_I = 64.0, 1.0 / 64.0
LAG_B, LAG_C, LAG_D = 2, 3, 4
AHEAD = 3


def _scale(val, s8):
    rows, cols = val.shape
    return (val.reshape(rows // 8, 8, cols) * s8[None]).reshape(rows, cols)


def _main_kernel(mask, eu0, ei0, tri, out_i, out_p, ua, id_u, id_p, id_n,
                 m8, stage, pan, snd_a, rcv_a, snd_b, rcv_b, xs, xr,
                 uacc, yr, raw, eus, cs, csr, sib, cacc, rs, rsum, rsum_r, su,
                 st_sem, ld_sem, agx_s, agx_r, agd_s, agd_r, agf_s, agf_r, cs_s, cs_r,
                 rs_s, rs_r, a_s, a_r, b_s, b_r, x_s, x_r, y_s, y_r, w_s, w_r, g_s, g_r, o_s, o_r, l_sem, p_sem):
    c = lax.axis_index("col")
    r = lax.axis_index("row")
    x = r // 2
    k = r % 2
    r_par = 2 * x + (1 - k)
    r_xp = 2 * (1 - x) + k
    r_xq = 2 * (1 - x) + (1 - k)
    par = (c, r_par)
    xpe = (c, r_xp)
    xpa = (c, r_xq)
    ype = (1 - c, r)

    def rcopy(src, dst, ss, rsm, dev):
        return pltpu.make_async_remote_copy(src_ref=src, dst_ref=dst, send_sem=ss, recv_sem=rsm,
                                            device_id=dev, device_id_type=MESH)

    def piece(p):
        blk = p // 4
        row = pl.multiple_of((p % 4) * PIECE, PIECE)
        col = pl.multiple_of((blk % 4) * QUART + (blk // 4) * CH, CH)
        return pltpu.make_async_copy(mask.at[pl.ds(row, PIECE), pl.ds(col, CH)],
                                     stage.at[p % RING], st_sem.at[p % RING])

    def own_load(j):
        return pltpu.make_async_copy(ei0.at[:, pl.ds(pl.multiple_of(j * CH, CH), CH)],
                                     pan.at[0, j * 4 + r], ld_sem.at[j])

    user_load = pltpu.make_async_copy(eu0, raw.at[0, c], ld_sem.at[NCH])
    for j in range(NCH):
        own_load(j).start()
    user_load.start()
    for p in range(RING):
        piece(p).start()

    barrier = pltpu.get_barrier_semaphore()
    for cc in range(2):
        for rr in range(4):
            pl.semaphore_signal(barrier, inc=1, device_id=(cc, rr), device_id_type=MESH)
    pl.semaphore_wait(barrier, 8)

    def ag_x(a, j, q):
        i = a * NCH + j
        ref = pan.at[a, j * 4 + q]
        return rcopy(ref, ref, agx_s.at[i], agx_r.at[i], xpe)

    def ag_d(a, j, q):
        i = a * NCH + j
        ref = pan.at[a, j * 4 + q]
        return rcopy(ref, ref, agd_s.at[i], agd_r.at[i], par)

    def ag_f(a, j, q):
        i = a * NCH + j
        ref = pan.at[a, j * 4 + q]
        return rcopy(ref, ref, agf_s.at[i], agf_r.at[i], par)

    for j in range(NCH):
        own_load(j).wait()
        if j < AHEAD:
            ag_x(0, j, r).start()
        ag_d(0, j, r).start()
    user_load.wait()
    w0 = rcopy(raw.at[0, c], raw.at[0, c], w_s.at[0], w_r.at[0], ype)
    w0.start()

    rs[...] = jnp.zeros_like(rs)
    uacc[...] = jnp.zeros_like(uacc)

    def cs_copy(rel, g, dev):
        return rcopy(cs.at[pl.ds(g * 4, 4)], csr.at[rel, pl.ds(g * 4, 4)], cs_s.at[rel, g], cs_r.at[rel, g], dev)

    def user_prod(a, b):
        es = _scale(pan[a, b].astype(F32), sib[b] * DN_U).astype(BF)
        got = lax.dot_general(es, m8[b], (((1,), (1,)), ((), ())), preferred_element_type=F32)
        uacc[0] += got[:, :HALF]
        uacc[1] += got[:, HALF:]

    def first_users(g):
        for rel, dev in ((0, par), (1, xpe), (2, xpa)):
            cs_copy(rel, g, dev).wait_recv()
        ag_d(0, g, r_par).wait_recv()
        ag_f(0, g, r_xq).wait_recv()

        @pl.loop(0, 4)
        def _(q):
            b = g * 4 + q
            deg = cs[b] + csr[0, b] + csr[1, b] + csr[2, b]
            sib[b] = jnp.broadcast_to(lax.rsqrt(jnp.maximum(deg, 1.0)), (8, CH))
            user_prod(0, b)

    cp_deg = rcopy(rsum, rsum_r, rs_s.at[0], rs_r.at[0], ype)

    @pl.loop(0, NCH)
    def _(g):
        @pl.loop(0, 4)
        def _(q):
            b = g * 4 + q
            cacc[...] = jnp.zeros_like(cacc)

            @pl.loop(0, 4)
            def _(s):
                p = b * 4 + s
                piece(p).wait()
                slot = p % RING

                @pl.loop(0, PIECE // STEP)
                def _(i):
                    rows = pl.ds(pl.multiple_of(i * STEP, STEP), STEP)
                    dst = pl.ds(pl.multiple_of(s * PIECE + i * STEP, STEP), STEP)
                    f = stage[slot, rows, :].astype(F32)
                    m8[b, dst, :] = f.astype(F8)
                    cacc[...] += jnp.sum(f.reshape(STEP // 8, 8, CH), axis=0)
                    part = f[:, :128]
                    for w in range(1, CH // 128):
                        part = part + f[:, w * 128:(w + 1) * 128]
                    rs[dst, :] += part

                @pl.when(p + RING < 4 * NBLK)
                def _():
                    piece(p + RING).start()

            cs[b] = jnp.sum(cacc[...], axis=0, keepdims=True)

        for rel, dev in ((0, par), (1, xpe), (2, xpa)):
            cs_copy(rel, g, dev).start()

        @pl.when(g + AHEAD < NCH)
        def _():
            ag_x(0, g + AHEAD, r).start()

        @pl.when(g == NCH - 1)
        def _():
            rsum[...] = lax.dot_general(jnp.ones((8, 128), BF), rs[...].astype(BF), (((1,), (1,)), ((), ())),
                                        preferred_element_type=F32)
            cp_deg.start()

        ag_x(0, g, r_xp).wait_recv()
        ag_f(0, g, r_xp).start()

    cp_deg.wait()
    w0.wait()
    deg_u = lax.rsqrt(jnp.maximum(rsum[...] + rsum_r[...], 1.0))
    su[0] = deg_u[:, :HALF]
    su[1] = deg_u[:, HALF:]

    def user_operand(lay):
        for h in range(2):
            eus[lay, :, h * HALF:(h + 1) * HALF] = _scale(raw[lay, h].astype(F32), su[h] * DN_I).astype(BF)

    user_operand(0)

    def prod(lay, b):
        return jnp.dot(eus[lay], m8[b], preferred_element_type=F32)

    def cp_a(g):
        return rcopy(snd_a.at[g % 2], rcv_a.at[g % 2], a_s.at[g % 2], a_r.at[g % 2], par)

    def cp_b(g):
        return rcopy(snd_b.at[g % 4], rcv_b.at[g % 4], b_s.at[g % 4], b_r.at[g % 4], par)

    def cp_x(g):
        return rcopy(xs.at[g % 4], xr.at[g % 8], x_s.at[g % 4], x_r.at[g % 8], xpe)

    def step_a(g):
        lay = g // NCH
        b = (g % NCH) * 4

        @pl.when(g >= 2)
        def _():
            cp_a(g - 2).wait_send()

        snd_a[g % 2] = prod(lay, b + r_xq)
        cp_a(g).start()

        @pl.when(g >= 4)
        def _():
            cp_x(g - 4).wait_send()

        xs[g % 4] = prod(lay, b + r_xp)
        cp_a(g).wait_recv()
        xs[g % 4] += rcv_a[g % 2]
        cp_x(g).start()

        @pl.when(g >= 4)
        def _():
            cp_b(g - 4).wait_send()

        snd_b[g % 4] = prod(lay, b + r_par)
        cp_b(g).start()

    def cp_o(j, q):
        ref = pan.at[1, j * 4 + q]
        return rcopy(ref, ref, o_s.at[j], o_r.at[j], par)

    def store(out, j, q, sem):
        return pltpu.make_async_copy(pan.at[1, j * 4 + q], out.at[:, pl.ds(pl.multiple_of(j * CH, CH), CH)], sem.at[j])

    def step_b(g):
        lay = g // NCH
        j = g % NCH
        b = j * 4 + r
        own = prod(lay, b)
        cp_b(g).wait_recv()
        own = own + rcv_b[g % 4]
        cp_x(g).wait_recv()
        emb = _scale(own + xr[g % 8], sib[b] * UP_I).astype(BF)

        @pl.when(lay < 2)
        def _():
            pan[lay + 1, b] = emb
            ag_x(lay + 1, j, r).start()
            ag_d(lay + 1, j, r).start()

        @pl.when(lay == 2)
        def _():
            tot = pan[0, b].astype(F32) + pan[1, b].astype(F32) + pan[2, b].astype(F32) + emb.astype(F32)
            ag_x(1, j, r).wait_send()
            ag_d(1, j, r).wait_send()
            pan[1, b] = (tot * 0.25).astype(BF)
            cp_o(j, r).start()
            store(out_i, j, r, l_sem).start()

            @pl.when(j >= 1)
            def _():
                cp_o(j - 1, r_par).wait_recv()
                store(out_p, j - 1, r_par, p_sem).start()

    def step_c(g):
        a = g // NCH + 1
        ag_x(a, g % NCH, r_xp).wait_recv()
        ag_f(a, g % NCH, r_xp).start()

    def step_d(g):
        a = g // NCH + 1
        j = g % NCH
        ag_d(a, j, r_par).wait_recv()
        ag_f(a, j, r_xq).wait_recv()

        @pl.loop(0, 4)
        def _(q):
            user_prod(a, j * 4 + q)

    def cp_y(lay):
        return rcopy(uacc.at[1 - c], yr.at[lay - 1], y_s.at[lay - 1], y_r.at[lay - 1], ype)

    def cp_w(lay):
        return rcopy(raw.at[lay, c], raw.at[lay, c], w_s.at[lay], w_r.at[lay], ype)

    def user_emb(lay):
        cp_y(lay).wait()
        emb = _scale(uacc[c] + yr[lay - 1], su[c] * UP_U).astype(BF)
        uacc[...] = jnp.zeros_like(uacc)
        return emb

    def finish_user(lay):
        raw[lay, c] = user_emb(lay)
        cp_w(lay).start()

    def load_user(lay):
        cp_w(lay).wait()
        user_operand(lay)

    def cp_g(i, blk, dev):
        return rcopy(ua.at[blk], ua.at[blk], g_s.at[i], g_r.at[i], dev)

    own_u = 2 * r + c
    D1, D2 = NCH - 1 + LAG_D, 2 * NCH - 1 + LAG_D

    @pl.loop(0, LAYERS * NCH + LAG_B)
    def _(t):
        @pl.when(t < LAYERS * NCH)
        def _():
            step_a(t)

        @pl.when(t < 4)
        def _():
            first_users(2 * t)
            first_users(2 * t + 1)

        @pl.when(t == 3)
        def _():
            cp_y(1).start()

        @pl.when(t == 4)
        def _():
            finish_user(1)
            for i in range(32):
                for w, ids in enumerate((id_u, id_p, id_n)):
                    ids[i:i + 1, :] = tri[w:w + 1, i * 128:(i + 1) * 128] & ((4096 if w == 0 else 2 * QUART) - 1)

        @pl.when(t == 5)
        def _():
            load_user(1)

        @pl.when(t == D1 + 1)
        def _():
            finish_user(2)

        @pl.when(t == D1 + 2)
        def _():
            load_user(2)

        @pl.when(t == D2 + 1)
        def _():
            emb = user_emb(3).astype(F32)
            tot = raw[0, c].astype(F32) + raw[1, c].astype(F32) + raw[2, c].astype(F32) + emb
            ua[own_u] = (tot * 0.25).astype(BF)
            cp_g(0, own_u, ype).start()
            cp_g(1, own_u, par).start()
            cp_g(2, own_u, xpe).start()

        @pl.when(t == D2 + 2)
        def _():
            cp_g(0, 2 * r + 1 - c, ype).wait_recv()
            cp_g(1, 2 * r_par + c, par).wait_recv()
            cp_g(2, 2 * r_xp + c, xpe).wait_recv()
            cp_g(3, 2 * r + 1 - c, par).start()
            cp_g(4, 2 * r_xp + c, par).start()
            cp_g(5, 2 * r_xp + c, ype).start()

        @pl.when(t == D2 + 3)
        def _():
            cp_g(3, 2 * r_par + 1 - c, par).wait_recv()
            cp_g(4, 2 * r_xq + c, par).wait_recv()
            cp_g(5, 2 * r_xp + 1 - c, ype).wait_recv()
            cp_g(6, 2 * r_xp + 1 - c, par).start()

        @pl.when(t == D2 + 4)
        def _():
            cp_g(6, 2 * r_xq + 1 - c, par).wait_recv()

        @pl.when(t >= LAG_B)
        def _():
            step_b(t - LAG_B)

        @pl.when((t >= LAG_C) & (t < 2 * NCH + LAG_C))
        def _():
            step_c(t - LAG_C)

        @pl.when((t >= LAG_D) & (t < 2 * NCH + LAG_D))
        def _():
            step_d(t - LAG_D)

        @pl.when(t == D1)
        def _():
            cp_y(2).start()

        @pl.when(t == D2)
        def _():
            cp_y(3).start()

    cp_o(NCH - 1, r_par).wait_recv()
    store(out_p, NCH - 1, r_par, p_sem).start()

    last = LAYERS * NCH
    for g in range(last - 2, last):
        cp_a(g).wait_send()
    for g in range(last - 4, last):
        cp_b(g).wait_send()
    for g in range(last - 4, last):
        cp_x(g).wait_send()
    for i in range(7):
        cp_g(i, own_u, par).wait_send()

    @pl.loop(0, NCH)
    def _(j):
        for rel, dev in ((0, par), (1, xpe), (2, xpa)):
            cs_copy(rel, j, dev).wait_send()
        cp_o(j, r).wait_send()
        store(out_i, j, r, l_sem).wait()
        store(out_p, j, r_par, p_sem).wait()

    @pl.loop(0, 3 * NCH)
    def _(i):
        @pl.when(i // NCH != 1)
        def _():
            ag_x(i // NCH, i % NCH, r).wait_send()
            ag_d(i // NCH, i % NCH, r).wait_send()

        ag_f(i // NCH, i % NCH, r_xp).wait_send()


def _main(mask, eu0, ei0, tri):
    dma = pltpu.SemaphoreType.DMA
    any_spec = pl.BlockSpec(memory_space=pl.ANY)
    vmem = pl.BlockSpec(memory_space=pltpu.VMEM)
    return pl.pallas_call(
        _main_kernel,
        out_shape=(jax.ShapeDtypeStruct((EMB, QUART), BF), jax.ShapeDtypeStruct((EMB, QUART), BF),
                   jax.ShapeDtypeStruct((8, EMB, HALF), BF), *[jax.ShapeDtypeStruct((32, 128), jnp.int32)] * 3),
        in_specs=[any_spec, any_spec, any_spec, vmem],
        out_specs=(any_spec, any_spec, vmem, vmem, vmem, vmem),
        scratch_shapes=[
            pltpu.VMEM((NBLK, USERS, CH), F8),
            pltpu.VMEM((RING, PIECE, CH), jnp.int32),
            pltpu.VMEM((3, NBLK, EMB, CH), BF),
            pltpu.VMEM((2, EMB, CH), F32), pltpu.VMEM((2, EMB, CH), F32),
            pltpu.VMEM((4, EMB, CH), F32), pltpu.VMEM((4, EMB, CH), F32),
            pltpu.VMEM((4, EMB, CH), F32), pltpu.VMEM((8, EMB, CH), F32),
            pltpu.VMEM((2, EMB, HALF), F32), pltpu.VMEM((3, EMB, HALF), F32),
            pltpu.VMEM((3, 2, EMB, HALF), BF), pltpu.VMEM((3, EMB, USERS), BF),
            pltpu.VMEM((NBLK, 1, CH), F32), pltpu.VMEM((3, NBLK, 1, CH), F32),
            pltpu.VMEM((NBLK, 8, CH), F32), pltpu.VMEM((8, CH), F32),
            pltpu.VMEM((USERS, 128), F32), pltpu.VMEM((8, USERS), F32), pltpu.VMEM((8, USERS), F32),
            pltpu.VMEM((2, 8, HALF), F32),
            dma((RING,)), dma((NCH + 1,)),
            dma((3 * NCH,)), dma((3 * NCH,)), dma((3 * NCH,)), dma((3 * NCH,)), dma((3 * NCH,)), dma((3 * NCH,)),
            dma((3, NCH)), dma((3, NCH)), dma((1,)), dma((1,)),
            dma((2,)), dma((2,)), dma((4,)), dma((4,)), dma((4,)), dma((8,)),
            dma((3,)), dma((3,)), dma((3,)), dma((3,)), dma((7,)), dma((7,)), dma((NCH,)), dma((NCH,)), dma((NCH,)), dma((NCH,)),
        ],
        compiler_params=pltpu.CompilerParams(collective_id=0, has_side_effects=True, vmem_limit_bytes=67043328),
        name="propagate",
    )(mask, eu0, ei0, tri)


def _lookup_kernel(uid, pid, nid, tri, items, items_p, users, part, out_i, out_u, it, ut, pp, pn):
    c = lax.axis_index("col")
    r = lax.axis_index("row")
    k = r % 2
    out_i[...] = items[...]
    out_u[...] = users[2 * r + c]
    for src, at in ((items, k * QUART), (items_p, (1 - k) * QUART)):
        for i in range(QUART // 512):
            rows = pl.ds(pl.multiple_of(at + i * 512, 512), 512)
            it[rows, :EMB] = src[:, i * 512:(i + 1) * 512].astype(F32).T
    for i in range(8):
        ut[i * HALF:(i + 1) * HALF, :EMB] = users[i].astype(F32).T

    @pl.loop(0, 2048 // 64)
    def _(i):
        for w in range(64):
            t = i * 64 + w
            g = k * 2048 + t
            u = ut[pl.ds(uid[g], 1), :]
            pp[pl.ds(t, 1), :] = u * it[pl.ds(pid[g], 1), :]
            pn[pl.ds(t, 1), :] = u * it[pl.ds(nid[g], 1), :]

    @pl.loop(0, 4)
    def _(i):
        for w in range(4):
            at = i * 4 + w
            rows = pl.ds(pl.multiple_of(at * 128, 128), 128)
            cols = pl.ds(pl.multiple_of(k * 2048 + at * 128, 128), 128)
            sp = jnp.sum(pp[rows, :].T[:EMB], axis=0, keepdims=True)
            sn = jnp.sum(pn[rows, :].T[:EMB], axis=0, keepdims=True)
            own_p = tri[1:2, cols] // (2 * QUART) == 2 * c + r // 2
            own_n = tri[2:3, cols] // (2 * QUART) == 2 * c + r // 2
            part[pl.ds(at, 1), :] = jnp.where(own_p, sp, 0.0) - jnp.where(own_n, sn, 0.0)


def _lookup(ids, tri, items, items_p, users):
    vmem = pl.BlockSpec(memory_space=pltpu.VMEM)
    smem = pl.BlockSpec(memory_space=pltpu.SMEM)
    return pl.pallas_call(
        _lookup_kernel,
        out_shape=(jax.ShapeDtypeStruct((16, 128), F32), jax.ShapeDtypeStruct((EMB, QUART), BF),
                   jax.ShapeDtypeStruct((EMB, HALF), BF)),
        in_specs=[smem, smem, smem, vmem, vmem, vmem, vmem],
        out_specs=(vmem, vmem, vmem),
        scratch_shapes=[pltpu.VMEM((2 * QUART, 128), F32), pltpu.VMEM((4096, 128), F32),
                        pltpu.VMEM((2048, 128), F32), pltpu.VMEM((2048, 128), F32)],
        name="lookup",
    )(*[i.reshape(4096) for i in ids], tri, items, items_p, users)


def _loss_kernel(part, out, got, s_sem, r_sem):
    c = lax.axis_index("col")
    r = lax.axis_index("row")
    me = 2 * r + c
    barrier = pltpu.get_barrier_semaphore()
    for cc in range(2):
        for rr in range(4):
            pl.semaphore_signal(barrier, inc=1, device_id=(cc, rr), device_id_type=MESH)
    pl.semaphore_wait(barrier, 8)

    def copy(i, slot):
        dr, dc = i // 2, i % 2
        return pltpu.make_async_remote_copy(
            src_ref=part, dst_ref=got.at[slot], send_sem=s_sem.at[i], recv_sem=r_sem.at[i],
            device_id=((c + dc) % 2, (r + dr) % 4), device_id_type=MESH)

    def sender(i):
        return 2 * ((r + 4 - i // 2) % 4) + (c + i % 2) % 2

    for i in range(1, 8):
        copy(i, me).start()
    got[me] = part[...]
    for i in range(1, 8):
        copy(i, sender(i)).wait()
    for h in range(2):
        m = (got[2 * h] + got[2 * h + 1]) + (got[2 * h + 4] + got[2 * h + 5])
        out[h * 16:(h + 1) * 16, :] = jnp.maximum(-m, 0.0) + jnp.log1p(jnp.exp(-jnp.abs(m)))


def _loss(part):
    vmem = pl.BlockSpec(memory_space=pltpu.VMEM)
    return pl.pallas_call(
        _loss_kernel,
        out_shape=jax.ShapeDtypeStruct((32, 128), F32),
        in_specs=[vmem],
        out_specs=vmem,
        scratch_shapes=[pltpu.VMEM((8, 16, 128), F32), pltpu.SemaphoreType.DMA((8,)), pltpu.SemaphoreType.DMA((8,))],
        compiler_params=pltpu.CompilerParams(collective_id=1, has_side_effects=True),
        name="loss",
    )(part)


def solution(mesh):
    def device_body(mask_blk, user_shard, item_shard, triples):
        tri = triples.T
        out_it, par_it, users, *ids = _main(mask_blk, user_shard.T, item_shard.T, tri)
        part, out_it, out_ut = _lookup(ids, tri, out_it, par_it, users)
        bpr_loss = _loss(part).reshape(4096)
        return out_ut.T, out_it.T, bpr_loss

    return jax.shard_map(
        device_body,
        mesh=mesh,
        in_specs=(P("row", "col"), P(("row", "col"), None), P(("col", "row"), None), P()),
        out_specs=(P(("row", "col"), None), P(("col", "row"), None), P()),
        check_vma=False,
    )
```

```python
import jax
import jax.numpy as jnp
from jax import lax
from jax.experimental import pallas as pl
from jax.experimental.pallas import tpu as pltpu
from jax.sharding import PartitionSpec as P

LAYERS = 3
F8 = jnp.float8_e4m3fn
BF = jnp.bfloat16
F32 = jnp.float32
MESH = pl.DeviceIdType.MESH

EMB = 64
USERS = 1024
HALF = 512
QUART = 8192
CH = 1024
NCH = 8
NBLK = 32
PIECE = 256
STEP = 64
RING = 7
UP_U, DN_U = 256.0, 1.0 / 256.0
UP_I, DN_I = 64.0, 1.0 / 64.0
LAG_B, LAG_C, LAG_D = 2, 3, 4
AHEAD = 3


def _scale(val, s8):
    rows, cols = val.shape
    return (val.reshape(rows // 8, 8, cols) * s8[None]).reshape(rows, cols)


def _main_kernel(mask, eu0, ei0, tri_in, out_i, out_p, ua, id_u, id_p, id_n,
                 m8, stage, pan, snd_a, rcv_a, snd_b, rcv_b, xs, xr,
                 uacc, yr, raw, eus, cs, csr, sib, cacc, rs, rsum, rsum_r, su,
                 st_sem, ld_sem, agx_s, agx_r, agd_s, agd_r, agf_s, agf_r, cs_s, cs_r,
                 rs_s, rs_r, a_s, a_r, b_s, b_r, x_s, x_r, y_s, y_r, w_s, w_r, g_s, g_r, o_s, o_r, l_sem, tri):
    c = lax.axis_index("col")
    r = lax.axis_index("row")
    x = r // 2
    k = r % 2
    r_par = 2 * x + (1 - k)
    r_xp = 2 * (1 - x) + k
    r_xq = 2 * (1 - x) + (1 - k)
    par = (c, r_par)
    xpe = (c, r_xp)
    xpa = (c, r_xq)
    ype = (1 - c, r)

    def rcopy(src, dst, ss, rsm, dev):
        return pltpu.make_async_remote_copy(src_ref=src, dst_ref=dst, send_sem=ss, recv_sem=rsm,
                                            device_id=dev, device_id_type=MESH)

    def piece(p):
        blk = p // 4
        row = pl.multiple_of((p % 4) * PIECE, PIECE)
        col = pl.multiple_of((blk % 4) * QUART + (blk // 4) * CH, CH)
        return pltpu.make_async_copy(mask.at[pl.ds(row, PIECE), pl.ds(col, CH)],
                                     stage.at[p % RING], st_sem.at[p % RING])

    def own_load(j):
        return pltpu.make_async_copy(ei0.at[:, pl.ds(pl.multiple_of(j * CH, CH), CH)],
                                     pan.at[0, j * 4 + r], ld_sem.at[j])

    user_load = pltpu.make_async_copy(eu0, raw.at[0, c], ld_sem.at[NCH])
    tri_load = pltpu.make_async_copy(tri_in, tri, ld_sem.at[NCH + 1])
    for j in range(NCH):
        own_load(j).start()
    user_load.start()
    for p in range(RING):
        piece(p).start()
    tri_load.start()

    barrier = pltpu.get_barrier_semaphore()
    for cc in range(2):
        for rr in range(4):
            pl.semaphore_signal(barrier, inc=1, device_id=(cc, rr), device_id_type=MESH)
    pl.semaphore_wait(barrier, 8)

    def ag_x(a, j, q):
        i = a * NCH + j
        ref = pan.at[a, j * 4 + q]
        return rcopy(ref, ref, agx_s.at[i], agx_r.at[i], xpe)

    def ag_d(a, j, q):
        i = a * NCH + j
        ref = pan.at[a, j * 4 + q]
        return rcopy(ref, ref, agd_s.at[i], agd_r.at[i], par)

    def ag_f(a, j, q):
        i = a * NCH + j
        ref = pan.at[a, j * 4 + q]
        return rcopy(ref, ref, agf_s.at[i], agf_r.at[i], par)

    for j in range(NCH):
        own_load(j).wait()
        if j < AHEAD:
            ag_x(0, j, r).start()
        ag_d(0, j, r).start()
    user_load.wait()
    w0 = rcopy(raw.at[0, c], raw.at[0, c], w_s.at[0], w_r.at[0], ype)
    w0.start()

    rs[...] = jnp.zeros_like(rs)
    uacc[...] = jnp.zeros_like(uacc)

    def cs_copy(rel, g, dev):
        return rcopy(cs.at[pl.ds(g * 4, 4)], csr.at[rel, pl.ds(g * 4, 4)], cs_s.at[rel, g], cs_r.at[rel, g], dev)

    def user_prod(a, b):
        es = _scale(pan[a, b].astype(F32), sib[b] * DN_U).astype(BF)
        got = lax.dot_general(es, m8[b], (((1,), (1,)), ((), ())), preferred_element_type=F32)
        uacc[0] += got[:, :HALF]
        uacc[1] += got[:, HALF:]

    def first_users(g):
        for rel, dev in ((0, par), (1, xpe), (2, xpa)):
            cs_copy(rel, g, dev).wait_recv()
        ag_d(0, g, r_par).wait_recv()
        ag_f(0, g, r_xq).wait_recv()

        @pl.loop(0, 4)
        def _(q):
            b = g * 4 + q
            deg = cs[b] + csr[0, b] + csr[1, b] + csr[2, b]
            sib[b] = jnp.broadcast_to(lax.rsqrt(jnp.maximum(deg, 1.0)), (8, CH))
            user_prod(0, b)

    cp_deg = rcopy(rsum, rsum_r, rs_s.at[0], rs_r.at[0], ype)

    @pl.loop(0, NCH)
    def _(g):
        @pl.loop(0, 4)
        def _(q):
            b = g * 4 + q
            cacc[...] = jnp.zeros_like(cacc)

            @pl.loop(0, 4)
            def _(s):
                p = b * 4 + s
                piece(p).wait()
                slot = p % RING

                @pl.loop(0, PIECE // STEP)
                def _(i):
                    rows = pl.ds(pl.multiple_of(i * STEP, STEP), STEP)
                    dst = pl.ds(pl.multiple_of(s * PIECE + i * STEP, STEP), STEP)
                    f = stage[slot, rows, :].astype(F32)
                    m8[b, dst, :] = f.astype(F8)
                    cacc[...] += jnp.sum(f.reshape(STEP // 8, 8, CH), axis=0)
                    part = f[:, :128]
                    for w in range(1, CH // 128):
                        part = part + f[:, w * 128:(w + 1) * 128]
                    rs[dst, :] += part

                @pl.when(p + RING < 4 * NBLK)
                def _():
                    piece(p + RING).start()

            cs[b] = jnp.sum(cacc[...], axis=0, keepdims=True)

        for rel, dev in ((0, par), (1, xpe), (2, xpa)):
            cs_copy(rel, g, dev).start()

        @pl.when(g + AHEAD < NCH)
        def _():
            ag_x(0, g + AHEAD, r).start()

        @pl.when(g == NCH - 1)
        def _():
            rsum[...] = lax.dot_general(jnp.ones((8, 128), BF), rs[...].astype(BF), (((1,), (1,)), ((), ())),
                                        preferred_element_type=F32)
            cp_deg.start()

        ag_x(0, g, r_xp).wait_recv()
        ag_f(0, g, r_xp).start()

    cp_deg.wait()
    w0.wait()
    deg_u = lax.rsqrt(jnp.maximum(rsum[...] + rsum_r[...], 1.0))
    su[0] = deg_u[:, :HALF]
    su[1] = deg_u[:, HALF:]

    def user_operand(lay):
        for h in range(2):
            eus[lay, :, h * HALF:(h + 1) * HALF] = _scale(raw[lay, h].astype(F32), su[h] * DN_I).astype(BF)

    user_operand(0)

    def prod(lay, b):
        return jnp.dot(eus[lay], m8[b], preferred_element_type=F32)

    def cp_a(g):
        return rcopy(snd_a.at[g % 2], rcv_a.at[g % 2], a_s.at[g % 2], a_r.at[g % 2], par)

    def cp_b(g):
        return rcopy(snd_b.at[g % 4], rcv_b.at[g % 4], b_s.at[g % 4], b_r.at[g % 4], par)

    def cp_x(g):
        return rcopy(xs.at[g % 4], xr.at[g % 8], x_s.at[g % 4], x_r.at[g % 8], xpe)

    def step_a(g):
        lay = g // NCH
        b = (g % NCH) * 4

        @pl.when(g >= 2)
        def _():
            cp_a(g - 2).wait_send()

        snd_a[g % 2] = prod(lay, b + r_xq)
        cp_a(g).start()

        @pl.when(g >= 4)
        def _():
            cp_x(g - 4).wait_send()

        xs[g % 4] = prod(lay, b + r_xp)
        cp_a(g).wait_recv()
        xs[g % 4] += rcv_a[g % 2]
        cp_x(g).start()

        @pl.when(g >= 4)
        def _():
            cp_b(g - 4).wait_send()

        snd_b[g % 4] = prod(lay, b + r_par)
        cp_b(g).start()

    def cp_o(j, q):
        return rcopy(pan.at[1, j * 4 + q], out_p.at[:, pl.ds(pl.multiple_of(j * CH, CH), CH)], o_s.at[j], o_r.at[j], par)

    def store(j):
        return pltpu.make_async_copy(pan.at[1, j * 4 + r], out_i.at[:, pl.ds(pl.multiple_of(j * CH, CH), CH)], l_sem.at[j])

    def step_b(g):
        lay = g // NCH
        j = g % NCH
        b = j * 4 + r
        own = prod(lay, b)
        cp_b(g).wait_recv()
        own = own + rcv_b[g % 4]
        cp_x(g).wait_recv()
        emb = _scale(own + xr[g % 8], sib[b] * UP_I).astype(BF)

        @pl.when(lay < 2)
        def _():
            pan[lay + 1, b] = emb
            ag_x(lay + 1, j, r).start()
            ag_d(lay + 1, j, r).start()

        @pl.when(lay == 2)
        def _():
            tot = pan[0, b].astype(F32) + pan[1, b].astype(F32) + pan[2, b].astype(F32) + emb.astype(F32)
            ag_x(1, j, r).wait_send()
            ag_d(1, j, r).wait_send()
            pan[1, b] = (tot * 0.25).astype(BF)
            cp_o(j, r).start()
            store(j).start()

    def step_c(g):
        a = g // NCH + 1
        ag_x(a, g % NCH, r_xp).wait_recv()
        ag_f(a, g % NCH, r_xp).start()

    def step_d(g):
        a = g // NCH + 1
        j = g % NCH
        ag_d(a, j, r_par).wait_recv()
        ag_f(a, j, r_xq).wait_recv()

        @pl.loop(0, 4)
        def _(q):
            user_prod(a, j * 4 + q)

    def cp_y(lay):
        return rcopy(uacc.at[1 - c], yr.at[lay - 1], y_s.at[lay - 1], y_r.at[lay - 1], ype)

    def cp_w(lay):
        return rcopy(raw.at[lay, c], raw.at[lay, c], w_s.at[lay], w_r.at[lay], ype)

    def user_emb(lay):
        cp_y(lay).wait()
        emb = _scale(uacc[c] + yr[lay - 1], su[c] * UP_U).astype(BF)
        uacc[...] = jnp.zeros_like(uacc)
        return emb

    def finish_user(lay):
        raw[lay, c] = user_emb(lay)
        cp_w(lay).start()

    def load_user(lay):
        cp_w(lay).wait()
        user_operand(lay)

    def cp_g(i, blk, dev):
        return rcopy(ua.at[blk], ua.at[blk], g_s.at[i], g_r.at[i], dev)

    own_u = 2 * r + c
    D1, D2 = NCH - 1 + LAG_D, 2 * NCH - 1 + LAG_D

    @pl.loop(0, LAYERS * NCH + LAG_B)
    def _(t):
        @pl.when(t < LAYERS * NCH)
        def _():
            step_a(t)

        @pl.when(t < 4)
        def _():
            first_users(2 * t)
            first_users(2 * t + 1)

        @pl.when(t == 3)
        def _():
            cp_y(1).start()

        @pl.when(t == 4)
        def _():
            finish_user(1)
            tri_load.wait()
            for i in range(32):
                for w, ids in enumerate((id_u, id_p, id_n)):
                    ids[i:i + 1, :] = tri[w:w + 1, i * 128:(i + 1) * 128] & ((4096 if w == 0 else 2 * QUART) - 1)

        @pl.when(t == 5)
        def _():
            load_user(1)

        @pl.when(t == D1 + 1)
        def _():
            finish_user(2)

        @pl.when(t == D1 + 2)
        def _():
            load_user(2)

        @pl.when(t == D2 + 1)
        def _():
            emb = user_emb(3).astype(F32)
            tot = raw[0, c].astype(F32) + raw[1, c].astype(F32) + raw[2, c].astype(F32) + emb
            ua[own_u] = (tot * 0.25).astype(BF)
            cp_g(0, own_u, ype).start()
            cp_g(1, own_u, par).start()
            cp_g(2, own_u, xpe).start()

        @pl.when(t == D2 + 2)
        def _():
            cp_g(0, 2 * r + 1 - c, ype).wait_recv()
            cp_g(1, 2 * r_par + c, par).wait_recv()
            cp_g(2, 2 * r_xp + c, xpe).wait_recv()
            cp_g(3, 2 * r + 1 - c, par).start()
            cp_g(4, 2 * r_xp + c, par).start()
            cp_g(5, 2 * r_xp + c, ype).start()

        @pl.when(t == D2 + 3)
        def _():
            cp_g(3, 2 * r_par + 1 - c, par).wait_recv()
            cp_g(4, 2 * r_xq + c, par).wait_recv()
            cp_g(5, 2 * r_xp + 1 - c, ype).wait_recv()
            cp_g(6, 2 * r_xp + 1 - c, par).start()

        @pl.when(t == D2 + 4)
        def _():
            cp_g(6, 2 * r_xq + 1 - c, par).wait_recv()

        @pl.when(t >= LAG_B)
        def _():
            step_b(t - LAG_B)

        @pl.when((t >= LAG_C) & (t < 2 * NCH + LAG_C))
        def _():
            step_c(t - LAG_C)

        @pl.when((t >= LAG_D) & (t < 2 * NCH + LAG_D))
        def _():
            step_d(t - LAG_D)

        @pl.when(t == D1)
        def _():
            cp_y(2).start()

        @pl.when(t == D2)
        def _():
            cp_y(3).start()

    last = LAYERS * NCH
    for g in range(last - 2, last):
        cp_a(g).wait_send()
    for g in range(last - 4, last):
        cp_b(g).wait_send()
    for g in range(last - 4, last):
        cp_x(g).wait_send()
    for i in range(7):
        cp_g(i, own_u, par).wait_send()

    @pl.loop(0, NCH)
    def _(j):
        for rel, dev in ((0, par), (1, xpe), (2, xpa)):
            cs_copy(rel, j, dev).wait_send()
        cp_o(j, r).wait()
        store(j).wait()

    @pl.loop(0, 3 * NCH)
    def _(i):
        @pl.when(i // NCH != 1)
        def _():
            ag_x(i // NCH, i % NCH, r).wait_send()
            ag_d(i // NCH, i % NCH, r).wait_send()

        ag_f(i // NCH, i % NCH, r_xp).wait_send()


def _main(mask, eu0, ei0, tri):
    dma = pltpu.SemaphoreType.DMA
    any_spec = pl.BlockSpec(memory_space=pl.ANY)
    vmem = pl.BlockSpec(memory_space=pltpu.VMEM)
    return pl.pallas_call(
        _main_kernel,
        out_shape=(jax.ShapeDtypeStruct((EMB, QUART), BF), jax.ShapeDtypeStruct((EMB, QUART), BF),
                   jax.ShapeDtypeStruct((8, EMB, HALF), BF), *[jax.ShapeDtypeStruct((32, 128), jnp.int32)] * 3),
        in_specs=[any_spec, any_spec, any_spec, any_spec],
        out_specs=(any_spec, any_spec, vmem, vmem, vmem, vmem),
        scratch_shapes=[
            pltpu.VMEM((NBLK, USERS, CH), F8),
            pltpu.VMEM((RING, PIECE, CH), jnp.int32),
            pltpu.VMEM((3, NBLK, EMB, CH), BF),
            pltpu.VMEM((2, EMB, CH), F32), pltpu.VMEM((2, EMB, CH), F32),
            pltpu.VMEM((4, EMB, CH), F32), pltpu.VMEM((4, EMB, CH), F32),
            pltpu.VMEM((4, EMB, CH), F32), pltpu.VMEM((8, EMB, CH), F32),
            pltpu.VMEM((2, EMB, HALF), F32), pltpu.VMEM((3, EMB, HALF), F32),
            pltpu.VMEM((3, 2, EMB, HALF), BF), pltpu.VMEM((3, EMB, USERS), BF),
            pltpu.VMEM((NBLK, 1, CH), F32), pltpu.VMEM((3, NBLK, 1, CH), F32),
            pltpu.VMEM((NBLK, 8, CH), F32), pltpu.VMEM((8, CH), F32),
            pltpu.VMEM((USERS, 128), F32), pltpu.VMEM((8, USERS), F32), pltpu.VMEM((8, USERS), F32),
            pltpu.VMEM((2, 8, HALF), F32),
            dma((RING,)), dma((NCH + 2,)),
            dma((3 * NCH,)), dma((3 * NCH,)), dma((3 * NCH,)), dma((3 * NCH,)), dma((3 * NCH,)), dma((3 * NCH,)),
            dma((3, NCH)), dma((3, NCH)), dma((1,)), dma((1,)),
            dma((2,)), dma((2,)), dma((4,)), dma((4,)), dma((4,)), dma((8,)),
            dma((3,)), dma((3,)), dma((3,)), dma((3,)), dma((7,)), dma((7,)), dma((NCH,)), dma((NCH,)), dma((NCH,)), pltpu.VMEM((3, 4096), jnp.int32),
        ],
        compiler_params=pltpu.CompilerParams(collective_id=0, has_side_effects=True, vmem_limit_bytes=67043328),
        name="propagate",
    )(mask, eu0, ei0, tri)


def _lookup_kernel(uid, pid, nid, tri, items, items_p, users_in, part, out_i, out_u, it, ut, pp, pn, vi, users, sem):
    c = lax.axis_index("col")
    r = lax.axis_index("row")
    k = r % 2
    loads = [pltpu.make_async_copy(users_in, users, sem.at[0]), pltpu.make_async_copy(items, vi.at[0], sem.at[1]),
             pltpu.make_async_copy(items_p, vi.at[1], sem.at[2])]
    for load in loads:
        load.start()
    put_u = pltpu.make_async_copy(users.at[2 * r + c], out_u, sem.at[3])
    put_i = pltpu.make_async_copy(vi.at[0], out_i, sem.at[4])
    loads[0].wait()
    put_u.start()
    for i in range(8):
        ut[i * HALF:(i + 1) * HALF, :EMB] = users[i].astype(F32).T
    for n, at in ((0, k * QUART), (1, (1 - k) * QUART)):
        loads[1 + n].wait()
        if n == 0:
            put_i.start()
        for i in range(QUART // 512):
            rows = pl.ds(pl.multiple_of(at + i * 512, 512), 512)
            it[rows, :EMB] = vi[n, :, i * 512:(i + 1) * 512].astype(F32).T

    @pl.loop(0, 2048 // 64)
    def _(i):
        for w in range(64):
            t = i * 64 + w
            g = k * 2048 + t
            u = ut[pl.ds(uid[g], 1), :]
            pp[pl.ds(t, 1), :] = u * it[pl.ds(pid[g], 1), :]
            pn[pl.ds(t, 1), :] = u * it[pl.ds(nid[g], 1), :]

    @pl.loop(0, 4)
    def _(i):
        for w in range(4):
            at = i * 4 + w
            rows = pl.ds(pl.multiple_of(at * 128, 128), 128)
            cols = pl.ds(pl.multiple_of(k * 2048 + at * 128, 128), 128)
            sp = jnp.sum(pp[rows, :].T[:EMB], axis=0, keepdims=True)
            sn = jnp.sum(pn[rows, :].T[:EMB], axis=0, keepdims=True)
            own_p = tri[1:2, cols] // (2 * QUART) == 2 * c + r // 2
            own_n = tri[2:3, cols] // (2 * QUART) == 2 * c + r // 2
            part[pl.ds(at, 1), :] = jnp.where(own_p, sp, 0.0) - jnp.where(own_n, sn, 0.0)

    put_u.wait()
    put_i.wait()


def _lookup(ids, tri, items, items_p, users):
    vmem = pl.BlockSpec(memory_space=pltpu.VMEM)
    smem = pl.BlockSpec(memory_space=pltpu.SMEM)
    any_spec = pl.BlockSpec(memory_space=pl.ANY)
    return pl.pallas_call(
        _lookup_kernel,
        out_shape=(jax.ShapeDtypeStruct((16, 128), F32), jax.ShapeDtypeStruct((EMB, QUART), BF),
                   jax.ShapeDtypeStruct((EMB, HALF), BF)),
        in_specs=[smem, smem, smem, vmem, any_spec, any_spec, any_spec],
        out_specs=(vmem, any_spec, any_spec),
        scratch_shapes=[pltpu.VMEM((2 * QUART, 128), F32), pltpu.VMEM((4096, 128), F32),
                        pltpu.VMEM((2048, 128), F32), pltpu.VMEM((2048, 128), F32),
                        pltpu.VMEM((2, EMB, QUART), BF), pltpu.VMEM((8, EMB, HALF), BF), pltpu.SemaphoreType.DMA((5,))],
        name="lookup",
    )(*[i.reshape(4096) for i in ids], tri, items, items_p, users)


def _loss_kernel(part, out, got, s_sem, r_sem):
    c = lax.axis_index("col")
    r = lax.axis_index("row")
    me = 2 * r + c
    barrier = pltpu.get_barrier_semaphore()
    for cc in range(2):
        for rr in range(4):
            pl.semaphore_signal(barrier, inc=1, device_id=(cc, rr), device_id_type=MESH)
    pl.semaphore_wait(barrier, 8)

    def copy(i, slot):
        dr, dc = i // 2, i % 2
        return pltpu.make_async_remote_copy(
            src_ref=part, dst_ref=got.at[slot], send_sem=s_sem.at[i], recv_sem=r_sem.at[i],
            device_id=((c + dc) % 2, (r + dr) % 4), device_id_type=MESH)

    def sender(i):
        return 2 * ((r + 4 - i // 2) % 4) + (c + i % 2) % 2

    for i in range(1, 8):
        copy(i, me).start()
    got[me] = part[...]
    for i in range(1, 8):
        copy(i, sender(i)).wait()
    for h in range(2):
        m = (got[2 * h] + got[2 * h + 1]) + (got[2 * h + 4] + got[2 * h + 5])
        out[h * 16:(h + 1) * 16, :] = jnp.maximum(-m, 0.0) + jnp.log1p(jnp.exp(-jnp.abs(m)))


def _loss(part):
    vmem = pl.BlockSpec(memory_space=pltpu.VMEM)
    return pl.pallas_call(
        _loss_kernel,
        out_shape=jax.ShapeDtypeStruct((32, 128), F32),
        in_specs=[vmem],
        out_specs=vmem,
        scratch_shapes=[pltpu.VMEM((8, 16, 128), F32), pltpu.SemaphoreType.DMA((8,)), pltpu.SemaphoreType.DMA((8,))],
        compiler_params=pltpu.CompilerParams(collective_id=1, has_side_effects=True),
        name="loss",
    )(part)


def solution(mesh):
    def device_body(mask_blk, user_shard, item_shard, triples):
        tri = triples.T
        out_it, par_it, users, *ids = _main(mask_blk, user_shard.T, item_shard.T, tri)
        part, out_it, out_ut = _lookup(ids, tri, out_it, par_it, users)
        bpr_loss = _loss(part).reshape(4096)
        return out_ut.T, out_it.T, bpr_loss

    return jax.shard_map(
        device_body,
        mesh=mesh,
        in_specs=(P("row", "col"), P(("row", "col"), None), P(("col", "row"), None), P()),
        out_specs=(P(("row", "col"), None), P(("col", "row"), None), P()),
        check_vma=False,
    )
```

```python
import jax
import jax.numpy as jnp
from jax import lax
from jax.experimental import pallas as pl
from jax.experimental.pallas import tpu as pltpu
from jax.sharding import PartitionSpec as P

LAYERS = 3
F8 = jnp.float8_e4m3fn
BF = jnp.bfloat16
F32 = jnp.float32
MESH = pl.DeviceIdType.MESH

EMB = 64
USERS = 1024
HALF = 512
QUART = 8192
CH = 1024
NCH = 8
NBLK = 32
PIECE = 256
STEP = 64
RING = 8
UP_U, DN_U = 256.0, 1.0 / 256.0
UP_I, DN_I = 64.0, 1.0 / 64.0
LAG_B, LAG_C, LAG_D = 2, 3, 4
AHEAD = 3


def _scale(val, s8):
    rows, cols = val.shape
    return (val.reshape(rows // 8, 8, cols) * s8[None]).reshape(rows, cols)


def _main_kernel(mask, eu0, ei0, tri_in, out_i, out_p, ua, id_u, id_p, id_n,
                 m8, stage, pan, snd_a, rcv_a, snd_b, rcv_b, xs, xr,
                 uacc, yr, raw, eus, cs, csr, sib, cacc, rs, rsum, rsum_r, su,
                 st_sem, ld_sem, agx_s, agx_r, agd_s, agd_r, agf_s, agf_r, cs_s, cs_r,
                 rs_s, rs_r, a_s, a_r, b_s, b_r, x_s, x_r, y_s, y_r, w_s, w_r, g_s, g_r, o_s, o_r, l_sem, tri):
    c = lax.axis_index("col")
    r = lax.axis_index("row")
    x = r // 2
    k = r % 2
    r_par = 2 * x + (1 - k)
    r_xp = 2 * (1 - x) + k
    r_xq = 2 * (1 - x) + (1 - k)
    par = (c, r_par)
    xpe = (c, r_xp)
    xpa = (c, r_xq)
    ype = (1 - c, r)

    def rcopy(src, dst, ss, rsm, dev):
        return pltpu.make_async_remote_copy(src_ref=src, dst_ref=dst, send_sem=ss, recv_sem=rsm,
                                            device_id=dev, device_id_type=MESH)

    def piece(p):
        blk = p // 4
        row = pl.multiple_of((p % 4) * PIECE, PIECE)
        col = pl.multiple_of((blk % 4) * QUART + (blk // 4) * CH, CH)
        return pltpu.make_async_copy(mask.at[pl.ds(row, PIECE), pl.ds(col, CH)],
                                     stage.at[p % RING], st_sem.at[p % RING])

    def own_load(j):
        return pltpu.make_async_copy(ei0.at[:, pl.ds(pl.multiple_of(j * CH, CH), CH)],
                                     pan.at[0, j * 4 + r], ld_sem.at[j])

    user_load = pltpu.make_async_copy(eu0, raw.at[0, c], ld_sem.at[NCH])
    tri_load = pltpu.make_async_copy(tri_in, tri, ld_sem.at[NCH + 1])
    for j in range(NCH):
        own_load(j).start()
    user_load.start()
    for p in range(RING):
        piece(p).start()
    tri_load.start()

    barrier = pltpu.get_barrier_semaphore()
    for cc in range(2):
        for rr in range(4):
            pl.semaphore_signal(barrier, inc=1, device_id=(cc, rr), device_id_type=MESH)
    pl.semaphore_wait(barrier, 8)

    def ag_x(a, j, q):
        i = a * NCH + j
        ref = pan.at[a, j * 4 + q]
        return rcopy(ref, ref, agx_s.at[i], agx_r.at[i], xpe)

    def ag_d(a, j, q):
        i = a * NCH + j
        ref = pan.at[a, j * 4 + q]
        return rcopy(ref, ref, agd_s.at[i], agd_r.at[i], par)

    def ag_f(a, j, q):
        i = a * NCH + j
        ref = pan.at[a, j * 4 + q]
        return rcopy(ref, ref, agf_s.at[i], agf_r.at[i], par)

    for j in range(NCH):
        own_load(j).wait()
        if j < AHEAD:
            ag_x(0, j, r).start()
        ag_d(0, j, r).start()
    user_load.wait()
    w0 = rcopy(raw.at[0, c], raw.at[0, c], w_s.at[0], w_r.at[0], ype)
    w0.start()

    rs[...] = jnp.zeros_like(rs)
    uacc[...] = jnp.zeros_like(uacc)

    def cs_copy(rel, g, dev):
        return rcopy(cs.at[pl.ds(g * 4, 4)], csr.at[rel, pl.ds(g * 4, 4)], cs_s.at[rel, g], cs_r.at[rel, g], dev)

    def user_prod(a, b):
        es = _scale(pan[a, b].astype(F32), sib[b] * DN_U).astype(BF)
        got = lax.dot_general(es, m8[b], (((1,), (1,)), ((), ())), preferred_element_type=F32)
        uacc[0] += got[:, :HALF]
        uacc[1] += got[:, HALF:]

    def first_users(g):
        for rel, dev in ((0, par), (1, xpe), (2, xpa)):
            cs_copy(rel, g, dev).wait_recv()
        ag_d(0, g, r_par).wait_recv()
        ag_f(0, g, r_xq).wait_recv()

        @pl.loop(0, 4)
        def _(q):
            b = g * 4 + q
            deg = cs[b] + csr[0, b] + csr[1, b] + csr[2, b]
            sib[b] = jnp.broadcast_to(lax.rsqrt(jnp.maximum(deg, 1.0)), (8, CH))
            user_prod(0, b)

    cp_deg = rcopy(rsum, rsum_r, rs_s.at[0], rs_r.at[0], ype)

    @pl.loop(0, NCH)
    def _(g):
        @pl.loop(0, 4)
        def _(q):
            b = g * 4 + q
            cacc[...] = jnp.zeros_like(cacc)

            @pl.loop(0, 4)
            def _(s):
                p = b * 4 + s
                piece(p).wait()
                slot = p % RING

                @pl.loop(0, PIECE // STEP)
                def _(i):
                    rows = pl.ds(pl.multiple_of(i * STEP, STEP), STEP)
                    dst = pl.ds(pl.multiple_of(s * PIECE + i * STEP, STEP), STEP)
                    f = stage[slot, rows, :].astype(F32)
                    m8[b, dst, :] = f.astype(F8)
                    cacc[...] += jnp.sum(f.reshape(STEP // 8, 8, CH), axis=0)
                    part = f[:, :128]
                    for w in range(1, CH // 128):
                        part = part + f[:, w * 128:(w + 1) * 128]
                    rs[dst, :] += part

                @pl.when(p + RING < 4 * NBLK)
                def _():
                    piece(p + RING).start()

            cs[b] = jnp.sum(cacc[...], axis=0, keepdims=True)

        @pl.when(g == NCH - 1)
        def _():
            rsum[...] = lax.dot_general(jnp.ones((8, 128), BF), rs[...].astype(BF), (((1,), (1,)), ((), ())),
                                        preferred_element_type=F32)
            cp_deg.start()

        for rel, dev in ((0, par), (1, xpe), (2, xpa)):
            cs_copy(rel, g, dev).start()

        @pl.when(g + AHEAD < NCH)
        def _():
            ag_x(0, g + AHEAD, r).start()

        @pl.when(g >= 1)
        def _():
            ag_x(0, g - 1, r_xp).wait_recv()
            ag_f(0, g - 1, r_xp).start()

    ag_x(0, NCH - 1, r_xp).wait_recv()
    ag_f(0, NCH - 1, r_xp).start()

    cp_deg.wait()
    w0.wait()
    deg_u = lax.rsqrt(jnp.maximum(rsum[...] + rsum_r[...], 1.0))
    su[0] = deg_u[:, :HALF]
    su[1] = deg_u[:, HALF:]

    def user_operand(lay):
        for h in range(2):
            eus[lay, :, h * HALF:(h + 1) * HALF] = _scale(raw[lay, h].astype(F32), su[h] * DN_I).astype(BF)

    user_operand(0)

    def prod(lay, b):
        return jnp.dot(eus[lay], m8[b], preferred_element_type=F32)

    def cp_a(g):
        return rcopy(snd_a.at[g % 2], rcv_a.at[g % 2], a_s.at[g % 2], a_r.at[g % 2], par)

    def cp_b(g):
        return rcopy(snd_b.at[g % 4], rcv_b.at[g % 4], b_s.at[g % 4], b_r.at[g % 4], par)

    def cp_x(g):
        return rcopy(xs.at[g % 4], xr.at[g % 8], x_s.at[g % 4], x_r.at[g % 8], xpe)

    def step_a(g):
        lay = g // NCH
        b = (g % NCH) * 4

        @pl.when(g >= 2)
        def _():
            cp_a(g - 2).wait_send()

        snd_a[g % 2] = prod(lay, b + r_xq)
        cp_a(g).start()

        @pl.when(g >= 4)
        def _():
            cp_x(g - 4).wait_send()

        xs[g % 4] = prod(lay, b + r_xp)
        cp_a(g).wait_recv()
        xs[g % 4] += rcv_a[g % 2]
        cp_x(g).start()

        @pl.when(g >= 4)
        def _():
            cp_b(g - 4).wait_send()

        snd_b[g % 4] = prod(lay, b + r_par)
        cp_b(g).start()

    def cp_o(j, q):
        return rcopy(pan.at[1, j * 4 + q], out_p.at[:, pl.ds(pl.multiple_of(j * CH, CH), CH)], o_s.at[j], o_r.at[j], par)

    def store(j):
        return pltpu.make_async_copy(pan.at[1, j * 4 + r], out_i.at[:, pl.ds(pl.multiple_of(j * CH, CH), CH)], l_sem.at[j])

    def step_b(g):
        lay = g // NCH
        j = g % NCH
        b = j * 4 + r
        own = prod(lay, b)
        cp_b(g).wait_recv()
        own = own + rcv_b[g % 4]
        cp_x(g).wait_recv()
        emb = _scale(own + xr[g % 8], sib[b] * UP_I).astype(BF)

        @pl.when(lay < 2)
        def _():
            pan[lay + 1, b] = emb
            ag_x(lay + 1, j, r).start()
            ag_d(lay + 1, j, r).start()

        @pl.when(lay == 2)
        def _():
            tot = pan[0, b].astype(F32) + pan[1, b].astype(F32) + pan[2, b].astype(F32) + emb.astype(F32)
            ag_x(1, j, r).wait_send()
            ag_d(1, j, r).wait_send()
            pan[1, b] = (tot * 0.25).astype(BF)
            cp_o(j, r).start()
            store(j).start()

    def step_c(g):
        a = g // NCH + 1
        ag_x(a, g % NCH, r_xp).wait_recv()
        ag_f(a, g % NCH, r_xp).start()

    def step_d(g):
        a = g // NCH + 1
        j = g % NCH
        ag_d(a, j, r_par).wait_recv()
        ag_f(a, j, r_xq).wait_recv()

        @pl.loop(0, 4)
        def _(q):
            user_prod(a, j * 4 + q)

    def cp_y(lay):
        return rcopy(uacc.at[1 - c], yr.at[lay - 1], y_s.at[lay - 1], y_r.at[lay - 1], ype)

    def cp_w(lay):
        return rcopy(raw.at[lay, c], raw.at[lay, c], w_s.at[lay], w_r.at[lay], ype)

    def user_emb(lay):
        cp_y(lay).wait()
        emb = _scale(uacc[c] + yr[lay - 1], su[c] * UP_U).astype(BF)
        uacc[...] = jnp.zeros_like(uacc)
        return emb

    def finish_user(lay):
        raw[lay, c] = user_emb(lay)
        cp_w(lay).start()

    def load_user(lay):
        cp_w(lay).wait()
        user_operand(lay)

    def cp_g(i, blk, dev):
        return rcopy(ua.at[blk], ua.at[blk], g_s.at[i], g_r.at[i], dev)

    own_u = 2 * r + c
    D1, D2 = NCH - 1 + LAG_D, 2 * NCH - 1 + LAG_D

    @pl.loop(0, LAYERS * NCH + LAG_B)
    def _(t):
        @pl.when(t < LAYERS * NCH)
        def _():
            step_a(t)

        @pl.when(t < 4)
        def _():
            first_users(2 * t)
            first_users(2 * t + 1)

        @pl.when(t == 3)
        def _():
            cp_y(1).start()

        @pl.when(t == 4)
        def _():
            finish_user(1)
            tri_load.wait()
            for i in range(32):
                for w, ids in enumerate((id_u, id_p, id_n)):
                    ids[i:i + 1, :] = tri[w:w + 1, i * 128:(i + 1) * 128] & ((4096 if w == 0 else 2 * QUART) - 1)

        @pl.when(t == 5)
        def _():
            load_user(1)

        @pl.when(t == D1 + 1)
        def _():
            finish_user(2)

        @pl.when(t == D1 + 2)
        def _():
            load_user(2)

        @pl.when(t == D2 + 1)
        def _():
            emb = user_emb(3).astype(F32)
            tot = raw[0, c].astype(F32) + raw[1, c].astype(F32) + raw[2, c].astype(F32) + emb
            ua[own_u] = (tot * 0.25).astype(BF)
            cp_g(0, own_u, ype).start()
            cp_g(1, own_u, par).start()
            cp_g(2, own_u, xpe).start()

        @pl.when(t == D2 + 2)
        def _():
            cp_g(0, 2 * r + 1 - c, ype).wait_recv()
            cp_g(1, 2 * r_par + c, par).wait_recv()
            cp_g(2, 2 * r_xp + c, xpe).wait_recv()
            cp_g(3, 2 * r + 1 - c, par).start()
            cp_g(4, 2 * r_xp + c, par).start()
            cp_g(5, 2 * r_xp + c, ype).start()

        @pl.when(t == D2 + 3)
        def _():
            cp_g(3, 2 * r_par + 1 - c, par).wait_recv()
            cp_g(4, 2 * r_xq + c, par).wait_recv()
            cp_g(5, 2 * r_xp + 1 - c, ype).wait_recv()
            cp_g(6, 2 * r_xp + 1 - c, par).start()

        @pl.when(t == D2 + 4)
        def _():
            cp_g(6, 2 * r_xq + 1 - c, par).wait_recv()

        @pl.when(t >= LAG_B)
        def _():
            step_b(t - LAG_B)

        @pl.when((t >= LAG_C) & (t < 2 * NCH + LAG_C))
        def _():
            step_c(t - LAG_C)

        @pl.when((t >= LAG_D) & (t < 2 * NCH + LAG_D))
        def _():
            step_d(t - LAG_D)

        @pl.when(t == D1)
        def _():
            cp_y(2).start()

        @pl.when(t == D2)
        def _():
            cp_y(3).start()

    last = LAYERS * NCH
    for g in range(last - 2, last):
        cp_a(g).wait_send()
    for g in range(last - 4, last):
        cp_b(g).wait_send()
    for g in range(last - 4, last):
        cp_x(g).wait_send()
    for i in range(7):
        cp_g(i, own_u, par).wait_send()

    @pl.loop(0, NCH)
    def _(j):
        for rel, dev in ((0, par), (1, xpe), (2, xpa)):
            cs_copy(rel, j, dev).wait_send()
        cp_o(j, r).wait()
        store(j).wait()

    @pl.loop(0, 3 * NCH)
    def _(i):
        @pl.when(i // NCH != 1)
        def _():
            ag_x(i // NCH, i % NCH, r).wait_send()
            ag_d(i // NCH, i % NCH, r).wait_send()

        ag_f(i // NCH, i % NCH, r_xp).wait_send()


def _main(mask, eu0, ei0, tri):
    dma = pltpu.SemaphoreType.DMA
    any_spec = pl.BlockSpec(memory_space=pl.ANY)
    vmem = pl.BlockSpec(memory_space=pltpu.VMEM)
    return pl.pallas_call(
        _main_kernel,
        out_shape=(jax.ShapeDtypeStruct((EMB, QUART), BF), jax.ShapeDtypeStruct((EMB, QUART), BF),
                   jax.ShapeDtypeStruct((8, EMB, HALF), BF), *[jax.ShapeDtypeStruct((32, 128), jnp.int32)] * 3),
        in_specs=[any_spec, any_spec, any_spec, any_spec],
        out_specs=(any_spec, any_spec, vmem, vmem, vmem, vmem),
        scratch_shapes=[
            pltpu.VMEM((NBLK, USERS, CH), F8),
            pltpu.VMEM((RING, PIECE, CH), jnp.int32),
            pltpu.VMEM((3, NBLK, EMB, CH), BF),
            pltpu.VMEM((2, EMB, CH), F32), pltpu.VMEM((2, EMB, CH), F32),
            pltpu.VMEM((4, EMB, CH), F32), pltpu.VMEM((4, EMB, CH), F32),
            pltpu.VMEM((4, EMB, CH), F32), pltpu.VMEM((8, EMB, CH), F32),
            pltpu.VMEM((2, EMB, HALF), F32), pltpu.VMEM((3, EMB, HALF), F32),
            pltpu.VMEM((3, 2, EMB, HALF), BF), pltpu.VMEM((3, EMB, USERS), BF),
            pltpu.VMEM((NBLK, 1, CH), F32), pltpu.VMEM((3, NBLK, 1, CH), F32),
            pltpu.VMEM((NBLK, 8, CH), F32), pltpu.VMEM((8, CH), F32),
            pltpu.VMEM((USERS, 128), F32), pltpu.VMEM((8, USERS), F32), pltpu.VMEM((8, USERS), F32),
            pltpu.VMEM((2, 8, HALF), F32),
            dma((RING,)), dma((NCH + 2,)),
            dma((3 * NCH,)), dma((3 * NCH,)), dma((3 * NCH,)), dma((3 * NCH,)), dma((3 * NCH,)), dma((3 * NCH,)),
            dma((3, NCH)), dma((3, NCH)), dma((1,)), dma((1,)),
            dma((2,)), dma((2,)), dma((4,)), dma((4,)), dma((4,)), dma((8,)),
            dma((3,)), dma((3,)), dma((3,)), dma((3,)), dma((7,)), dma((7,)), dma((NCH,)), dma((NCH,)), dma((NCH,)), pltpu.VMEM((3, 4096), jnp.int32),
        ],
        compiler_params=pltpu.CompilerParams(collective_id=0, has_side_effects=True, vmem_limit_bytes=67043328),
        name="propagate",
    )(mask, eu0, ei0, tri)


def _lookup_kernel(uid, pid, nid, tri, items, items_p, users, part, out_i, out_u, it, ut, pp, pn):
    c = lax.axis_index("col")
    r = lax.axis_index("row")
    k = r % 2
    out_i[...] = items[...]
    out_u[...] = users[2 * r + c]
    for src, at in ((items, k * QUART), (items_p, (1 - k) * QUART)):
        for i in range(QUART // 512):
            rows = pl.ds(pl.multiple_of(at + i * 512, 512), 512)
            it[rows, :EMB] = src[:, i * 512:(i + 1) * 512].astype(F32).T
    for i in range(8):
        ut[i * HALF:(i + 1) * HALF, :EMB] = users[i].astype(F32).T

    @pl.loop(0, 2048 // 64)
    def _(i):
        for w in range(64):
            t = i * 64 + w
            g = k * 2048 + t
            u = ut[pl.ds(uid[g], 1), :]
            pp[pl.ds(t, 1), :] = u * it[pl.ds(pid[g], 1), :]
            pn[pl.ds(t, 1), :] = u * it[pl.ds(nid[g], 1), :]

    @pl.loop(0, 4)
    def _(i):
        for w in range(4):
            at = i * 4 + w
            rows = pl.ds(pl.multiple_of(at * 128, 128), 128)
            cols = pl.ds(pl.multiple_of(k * 2048 + at * 128, 128), 128)
            sp = jnp.sum(pp[rows, :].T[:EMB], axis=0, keepdims=True)
            sn = jnp.sum(pn[rows, :].T[:EMB], axis=0, keepdims=True)
            own_p = tri[1:2, cols] // (2 * QUART) == 2 * c + r // 2
            own_n = tri[2:3, cols] // (2 * QUART) == 2 * c + r // 2
            part[pl.ds(at, 1), :] = jnp.where(own_p, sp, 0.0) - jnp.where(own_n, sn, 0.0)


def _lookup(ids, tri, items, items_p, users):
    vmem = pl.BlockSpec(memory_space=pltpu.VMEM)
    smem = pl.BlockSpec(memory_space=pltpu.SMEM)
    return pl.pallas_call(
        _lookup_kernel,
        out_shape=(jax.ShapeDtypeStruct((16, 128), F32), jax.ShapeDtypeStruct((EMB, QUART), BF),
                   jax.ShapeDtypeStruct((EMB, HALF), BF)),
        in_specs=[smem, smem, smem, vmem, vmem, vmem, vmem],
        out_specs=(vmem, vmem, vmem),
        scratch_shapes=[pltpu.VMEM((2 * QUART, 128), F32), pltpu.VMEM((4096, 128), F32),
                        pltpu.VMEM((2048, 128), F32), pltpu.VMEM((2048, 128), F32)],
        name="lookup",
    )(*[i.reshape(4096) for i in ids], tri, items, items_p, users)


def _loss_kernel(part_in, out, got, part, s_sem, r_sem):
    c = lax.axis_index("col")
    r = lax.axis_index("row")
    me = 2 * r + c
    load = pltpu.make_async_copy(part_in, part, s_sem.at[0])
    load.start()
    barrier = pltpu.get_barrier_semaphore()
    for cc in range(2):
        for rr in range(4):
            pl.semaphore_signal(barrier, inc=1, device_id=(cc, rr), device_id_type=MESH)
    pl.semaphore_wait(barrier, 8)
    load.wait()

    def copy(i, slot):
        dr, dc = i // 2, i % 2
        return pltpu.make_async_remote_copy(
            src_ref=part, dst_ref=got.at[slot], send_sem=s_sem.at[i], recv_sem=r_sem.at[i],
            device_id=((c + dc) % 2, (r + dr) % 4), device_id_type=MESH)

    def sender(i):
        return 2 * ((r + 4 - i // 2) % 4) + (c + i % 2) % 2

    for i in range(1, 8):
        copy(i, me).start()
    got[me] = part[...]
    for i in range(1, 8):
        copy(i, sender(i)).wait()
    for h in range(2):
        m = (got[2 * h] + got[2 * h + 1]) + (got[2 * h + 4] + got[2 * h + 5])
        out[h * 16:(h + 1) * 16, :] = jnp.maximum(-m, 0.0) + jnp.log1p(jnp.exp(-jnp.abs(m)))


def _loss(part):
    vmem = pl.BlockSpec(memory_space=pltpu.VMEM)
    return pl.pallas_call(
        _loss_kernel,
        out_shape=jax.ShapeDtypeStruct((32, 128), F32),
        in_specs=[pl.BlockSpec(memory_space=pl.ANY)],
        out_specs=vmem,
        scratch_shapes=[pltpu.VMEM((8, 16, 128), F32), pltpu.VMEM((16, 128), F32), pltpu.SemaphoreType.DMA((8,)), pltpu.SemaphoreType.DMA((8,))],
        compiler_params=pltpu.CompilerParams(collective_id=1, has_side_effects=True),
        name="loss",
    )(part)


def solution(mesh):
    def device_body(mask_blk, user_shard, item_shard, triples):
        tri = triples.T
        out_it, par_it, users, *ids = _main(mask_blk, user_shard.T, item_shard.T, tri)
        part, out_it, out_ut = _lookup(ids, tri, out_it, par_it, users)
        bpr_loss = _loss(part).reshape(4096)
        return out_ut.T, out_it.T, bpr_loss

    return jax.shard_map(
        device_body,
        mesh=mesh,
        in_specs=(P("row", "col"), P(("row", "col"), None), P(("col", "row"), None), P()),
        out_specs=(P(("row", "col"), None), P(("col", "row"), None), P()),
        check_vma=False,
    )
```

```python
import jax
import jax.numpy as jnp
from jax import lax
from jax.experimental import pallas as pl
from jax.experimental.pallas import tpu as pltpu
from jax.sharding import PartitionSpec as P

LAYERS = 3
F8 = jnp.float8_e4m3fn
BF = jnp.bfloat16
F32 = jnp.float32
MESH = pl.DeviceIdType.MESH

EMB = 64
USERS = 1024
HALF = 512
QUART = 8192
CH = 1024
NCH = 8
NBLK = 32
PIECE = 256
STEP = 64
RING = 8
UP_U, DN_U = 256.0, 1.0 / 256.0
UP_I, DN_I = 64.0, 1.0 / 64.0
LAG_B, LAG_C, LAG_D = 2, 3, 4
AHEAD = 3


def _scale(val, s8):
    rows, cols = val.shape
    return (val.reshape(rows // 8, 8, cols) * s8[None]).reshape(rows, cols)


def _main_kernel(mask, eu0, ei0, tri_in, out_i, out_p, ua, id_u, id_p, id_n,
                 m8, stage, pan, snd_a, rcv_a, snd_b, rcv_b, xs, xr,
                 uacc, yr, raw, eus, cs, csr, sib, cacc, rs, rsum, rsum_r, su,
                 st_sem, ld_sem, agx_s, agx_r, agd_s, agd_r, agf_s, agf_r, cs_s, cs_r,
                 rs_s, rs_r, a_s, a_r, b_s, b_r, x_s, x_r, y_s, y_r, w_s, w_r, g_s, g_r, o_s, o_r, l_sem, tri):
    c = lax.axis_index("col")
    r = lax.axis_index("row")
    x = r // 2
    k = r % 2
    r_par = 2 * x + (1 - k)
    r_xp = 2 * (1 - x) + k
    r_xq = 2 * (1 - x) + (1 - k)
    par = (c, r_par)
    xpe = (c, r_xp)
    xpa = (c, r_xq)
    ype = (1 - c, r)

    def rcopy(src, dst, ss, rsm, dev):
        return pltpu.make_async_remote_copy(src_ref=src, dst_ref=dst, send_sem=ss, recv_sem=rsm,
                                            device_id=dev, device_id_type=MESH)

    def piece(p):
        blk = p // 4
        row = pl.multiple_of((p % 4) * PIECE, PIECE)
        col = pl.multiple_of((blk % 4) * QUART + (blk // 4) * CH, CH)
        return pltpu.make_async_copy(mask.at[pl.ds(row, PIECE), pl.ds(col, CH)],
                                     stage.at[p % RING], st_sem.at[p % RING])

    def own_load(j):
        return pltpu.make_async_copy(ei0.at[:, pl.ds(pl.multiple_of(j * CH, CH), CH)],
                                     pan.at[0, j * 4 + r], ld_sem.at[j])

    user_load = pltpu.make_async_copy(eu0, raw.at[0, c], ld_sem.at[NCH])
    tri_load = pltpu.make_async_copy(tri_in, tri, ld_sem.at[NCH + 1])
    for j in range(NCH):
        own_load(j).start()
    user_load.start()
    for p in range(RING):
        piece(p).start()
    tri_load.start()

    barrier = pltpu.get_barrier_semaphore()
    for cc in range(2):
        for rr in range(4):
            pl.semaphore_signal(barrier, inc=1, device_id=(cc, rr), device_id_type=MESH)

    def ag_x(a, j, q):
        i = a * NCH + j
        ref = pan.at[a, j * 4 + q]
        return rcopy(ref, ref, agx_s.at[i], agx_r.at[i], xpe)

    def ag_d(a, j, q):
        i = a * NCH + j
        ref = pan.at[a, j * 4 + q]
        return rcopy(ref, ref, agd_s.at[i], agd_r.at[i], par)

    def ag_f(a, j, q):
        i = a * NCH + j
        ref = pan.at[a, j * 4 + q]
        return rcopy(ref, ref, agf_s.at[i], agf_r.at[i], par)

    rs[...] = jnp.zeros_like(rs)
    uacc[...] = jnp.zeros_like(uacc)

    def cs_copy(rel, g, dev):
        return rcopy(cs.at[pl.ds(g * 4, 4)], csr.at[rel, pl.ds(g * 4, 4)], cs_s.at[rel, g], cs_r.at[rel, g], dev)

    def user_prod(a, b):
        es = _scale(pan[a, b].astype(F32), sib[b] * DN_U).astype(BF)
        got = lax.dot_general(es, m8[b], (((1,), (1,)), ((), ())), preferred_element_type=F32)
        uacc[0] += got[:, :HALF]
        uacc[1] += got[:, HALF:]

    def first_users(g):
        for rel, dev in ((0, par), (1, xpe), (2, xpa)):
            cs_copy(rel, g, dev).wait_recv()
        ag_d(0, g, r_par).wait_recv()
        ag_f(0, g, r_xq).wait_recv()

        @pl.loop(0, 4)
        def _(q):
            b = g * 4 + q
            deg = cs[b] + csr[0, b] + csr[1, b] + csr[2, b]
            sib[b] = jnp.broadcast_to(lax.rsqrt(jnp.maximum(deg, 1.0)), (8, CH))
            user_prod(0, b)

    cp_deg = rcopy(rsum, rsum_r, rs_s.at[0], rs_r.at[0], ype)

    def take_group(g):
        @pl.loop(0, 4)
        def _(q):
            b = g * 4 + q
            cacc[...] = jnp.zeros_like(cacc)

            @pl.loop(0, 4)
            def _(s):
                p = b * 4 + s
                piece(p).wait()
                slot = p % RING

                @pl.loop(0, PIECE // STEP)
                def _(i):
                    rows = pl.ds(pl.multiple_of(i * STEP, STEP), STEP)
                    dst = pl.ds(pl.multiple_of(s * PIECE + i * STEP, STEP), STEP)
                    f = stage[slot, rows, :].astype(F32)
                    m8[b, dst, :] = f.astype(F8)
                    cacc[...] += jnp.sum(f.reshape(STEP // 8, 8, CH), axis=0)
                    part = f[:, :128]
                    for w in range(1, CH // 128):
                        part = part + f[:, w * 128:(w + 1) * 128]
                    rs[dst, :] += part

                @pl.when(p + RING < 4 * NBLK)
                def _():
                    piece(p + RING).start()

            cs[b] = jnp.sum(cacc[...], axis=0, keepdims=True)

    take_group(0)
    pl.semaphore_wait(barrier, 8)
    for j in range(NCH):
        own_load(j).wait()
        if j < AHEAD:
            ag_x(0, j, r).start()
        ag_d(0, j, r).start()
    user_load.wait()
    w0 = rcopy(raw.at[0, c], raw.at[0, c], w_s.at[0], w_r.at[0], ype)
    w0.start()

    for rel, dev in ((0, par), (1, xpe), (2, xpa)):
        cs_copy(rel, 0, dev).start()
    ag_x(0, AHEAD, r).start()

    @pl.loop(1, NCH)
    def _(g):
        take_group(g)

        @pl.when(g == NCH - 1)
        def _():
            rsum[...] = lax.dot_general(jnp.ones((8, 128), BF), rs[...].astype(BF), (((1,), (1,)), ((), ())),
                                        preferred_element_type=F32)
            cp_deg.start()

        for rel, dev in ((0, par), (1, xpe), (2, xpa)):
            cs_copy(rel, g, dev).start()

        @pl.when(g + AHEAD < NCH)
        def _():
            ag_x(0, g + AHEAD, r).start()

        ag_x(0, g - 1, r_xp).wait_recv()
        ag_f(0, g - 1, r_xp).start()

    ag_x(0, NCH - 1, r_xp).wait_recv()
    ag_f(0, NCH - 1, r_xp).start()

    cp_deg.wait()
    w0.wait()
    deg_u = lax.rsqrt(jnp.maximum(rsum[...] + rsum_r[...], 1.0))
    su[0] = deg_u[:, :HALF]
    su[1] = deg_u[:, HALF:]

    def user_operand(lay):
        for h in range(2):
            eus[lay, :, h * HALF:(h + 1) * HALF] = _scale(raw[lay, h].astype(F32), su[h] * DN_I).astype(BF)

    user_operand(0)

    def prod(lay, b):
        return jnp.dot(eus[lay], m8[b], preferred_element_type=F32)

    def cp_a(g):
        return rcopy(snd_a.at[g % 2], rcv_a.at[g % 2], a_s.at[g % 2], a_r.at[g % 2], par)

    def cp_b(g):
        return rcopy(snd_b.at[g % 4], rcv_b.at[g % 4], b_s.at[g % 4], b_r.at[g % 4], par)

    def cp_x(g):
        return rcopy(xs.at[g % 4], xr.at[g % 8], x_s.at[g % 4], x_r.at[g % 8], xpe)

    def step_a(g):
        lay = g // NCH
        b = (g % NCH) * 4

        @pl.when(g >= 2)
        def _():
            cp_a(g - 2).wait_send()

        snd_a[g % 2] = prod(lay, b + r_xq)
        cp_a(g).start()

        @pl.when(g >= 4)
        def _():
            cp_x(g - 4).wait_send()

        xs[g % 4] = prod(lay, b + r_xp)
        cp_a(g).wait_recv()
        xs[g % 4] += rcv_a[g % 2]
        cp_x(g).start()

        @pl.when(g >= 4)
        def _():
            cp_b(g - 4).wait_send()

        snd_b[g % 4] = prod(lay, b + r_par)
        cp_b(g).start()

    def cp_o(j, q):
        return rcopy(pan.at[1, j * 4 + q], out_p.at[:, pl.ds(pl.multiple_of(j * CH, CH), CH)], o_s.at[j], o_r.at[j], par)

    def store(j):
        return pltpu.make_async_copy(pan.at[1, j * 4 + r], out_i.at[:, pl.ds(pl.multiple_of(j * CH, CH), CH)], l_sem.at[j])

    def step_b(g):
        lay = g // NCH
        j = g % NCH
        b = j * 4 + r
        own = prod(lay, b)
        cp_b(g).wait_recv()
        own = own + rcv_b[g % 4]
        cp_x(g).wait_recv()
        emb = _scale(own + xr[g % 8], sib[b] * UP_I).astype(BF)

        @pl.when(lay < 2)
        def _():
            pan[lay + 1, b] = emb
            ag_x(lay + 1, j, r).start()
            ag_d(lay + 1, j, r).start()

        @pl.when(lay == 2)
        def _():
            tot = pan[0, b].astype(F32) + pan[1, b].astype(F32) + pan[2, b].astype(F32) + emb.astype(F32)
            ag_x(1, j, r).wait_send()
            ag_d(1, j, r).wait_send()
            pan[1, b] = (tot * 0.25).astype(BF)
            cp_o(j, r).start()
            store(j).start()

    def step_c(g):
        a = g // NCH + 1
        ag_x(a, g % NCH, r_xp).wait_recv()
        ag_f(a, g % NCH, r_xp).start()

    def step_d(g):
        a = g // NCH + 1
        j = g % NCH
        ag_d(a, j, r_par).wait_recv()
        ag_f(a, j, r_xq).wait_recv()

        @pl.loop(0, 4)
        def _(q):
            user_prod(a, j * 4 + q)

    def cp_y(lay):
        return rcopy(uacc.at[1 - c], yr.at[lay - 1], y_s.at[lay - 1], y_r.at[lay - 1], ype)

    def cp_w(lay):
        return rcopy(raw.at[lay, c], raw.at[lay, c], w_s.at[lay], w_r.at[lay], ype)

    def user_emb(lay):
        cp_y(lay).wait()
        emb = _scale(uacc[c] + yr[lay - 1], su[c] * UP_U).astype(BF)
        uacc[...] = jnp.zeros_like(uacc)
        return emb

    def finish_user(lay):
        raw[lay, c] = user_emb(lay)
        cp_w(lay).start()

    def load_user(lay):
        cp_w(lay).wait()
        user_operand(lay)

    def cp_g(i, blk, dev):
        return rcopy(ua.at[blk], ua.at[blk], g_s.at[i], g_r.at[i], dev)

    own_u = 2 * r + c
    D1, D2 = NCH - 1 + LAG_D, 2 * NCH - 1 + LAG_D

    @pl.loop(0, LAYERS * NCH + LAG_B)
    def _(t):
        @pl.when(t < LAYERS * NCH)
        def _():
            step_a(t)

        @pl.when(t < 4)
        def _():
            first_users(2 * t)
            first_users(2 * t + 1)

        @pl.when(t == 3)
        def _():
            cp_y(1).start()

        @pl.when(t == 4)
        def _():
            finish_user(1)
            tri_load.wait()
            for i in range(32):
                for w, ids in enumerate((id_u, id_p, id_n)):
                    ids[i:i + 1, :] = tri[w:w + 1, i * 128:(i + 1) * 128] & ((4096 if w == 0 else 2 * QUART) - 1)

        @pl.when(t == 5)
        def _():
            load_user(1)

        @pl.when(t == D1 + 1)
        def _():
            finish_user(2)

        @pl.when(t == D1 + 2)
        def _():
            load_user(2)

        @pl.when(t == D2 + 1)
        def _():
            emb = user_emb(3).astype(F32)
            tot = raw[0, c].astype(F32) + raw[1, c].astype(F32) + raw[2, c].astype(F32) + emb
            ua[own_u] = (tot * 0.25).astype(BF)
            cp_g(0, own_u, ype).start()
            cp_g(1, own_u, par).start()
            cp_g(2, own_u, xpe).start()

        @pl.when(t == D2 + 2)
        def _():
            cp_g(0, 2 * r + 1 - c, ype).wait_recv()
            cp_g(1, 2 * r_par + c, par).wait_recv()
            cp_g(2, 2 * r_xp + c, xpe).wait_recv()
            cp_g(3, 2 * r + 1 - c, par).start()
            cp_g(4, 2 * r_xp + c, par).start()
            cp_g(5, 2 * r_xp + c, ype).start()

        @pl.when(t == D2 + 3)
        def _():
            cp_g(3, 2 * r_par + 1 - c, par).wait_recv()
            cp_g(4, 2 * r_xq + c, par).wait_recv()
            cp_g(5, 2 * r_xp + 1 - c, ype).wait_recv()
            cp_g(6, 2 * r_xp + 1 - c, par).start()

        @pl.when(t == D2 + 4)
        def _():
            cp_g(6, 2 * r_xq + 1 - c, par).wait_recv()

        @pl.when(t >= LAG_B)
        def _():
            step_b(t - LAG_B)

        @pl.when((t >= LAG_C) & (t < 2 * NCH + LAG_C))
        def _():
            step_c(t - LAG_C)

        @pl.when((t >= LAG_D) & (t < 2 * NCH + LAG_D))
        def _():
            step_d(t - LAG_D)

        @pl.when(t == D1)
        def _():
            cp_y(2).start()

        @pl.when(t == D2)
        def _():
            cp_y(3).start()

    last = LAYERS * NCH
    for g in range(last - 2, last):
        cp_a(g).wait_send()
    for g in range(last - 4, last):
        cp_b(g).wait_send()
    for g in range(last - 4, last):
        cp_x(g).wait_send()
    for i in range(7):
        cp_g(i, own_u, par).wait_send()

    @pl.loop(0, NCH)
    def _(j):
        for rel, dev in ((0, par), (1, xpe), (2, xpa)):
            cs_copy(rel, j, dev).wait_send()
        cp_o(j, r).wait()
        store(j).wait()

    @pl.loop(0, 3 * NCH)
    def _(i):
        @pl.when(i // NCH != 1)
        def _():
            ag_x(i // NCH, i % NCH, r).wait_send()
            ag_d(i // NCH, i % NCH, r).wait_send()

        ag_f(i // NCH, i % NCH, r_xp).wait_send()


def _main(mask, eu0, ei0, tri):
    dma = pltpu.SemaphoreType.DMA
    any_spec = pl.BlockSpec(memory_space=pl.ANY)
    vmem = pl.BlockSpec(memory_space=pltpu.VMEM)
    return pl.pallas_call(
        _main_kernel,
        out_shape=(jax.ShapeDtypeStruct((EMB, QUART), BF), jax.ShapeDtypeStruct((EMB, QUART), BF),
                   jax.ShapeDtypeStruct((8, EMB, HALF), BF), *[jax.ShapeDtypeStruct((32, 128), jnp.int32)] * 3),
        in_specs=[any_spec, any_spec, any_spec, any_spec],
        out_specs=(any_spec, any_spec, vmem, vmem, vmem, vmem),
        scratch_shapes=[
            pltpu.VMEM((NBLK, USERS, CH), F8),
            pltpu.VMEM((RING, PIECE, CH), jnp.int32),
            pltpu.VMEM((3, NBLK, EMB, CH), BF),
            pltpu.VMEM((2, EMB, CH), F32), pltpu.VMEM((2, EMB, CH), F32),
            pltpu.VMEM((4, EMB, CH), F32), pltpu.VMEM((4, EMB, CH), F32),
            pltpu.VMEM((4, EMB, CH), F32), pltpu.VMEM((8, EMB, CH), F32),
            pltpu.VMEM((2, EMB, HALF), F32), pltpu.VMEM((3, EMB, HALF), F32),
            pltpu.VMEM((3, 2, EMB, HALF), BF), pltpu.VMEM((3, EMB, USERS), BF),
            pltpu.VMEM((NBLK, 1, CH), F32), pltpu.VMEM((3, NBLK, 1, CH), F32),
            pltpu.VMEM((NBLK, 8, CH), F32), pltpu.VMEM((8, CH), F32),
            pltpu.VMEM((USERS, 128), F32), pltpu.VMEM((8, USERS), F32), pltpu.VMEM((8, USERS), F32),
            pltpu.VMEM((2, 8, HALF), F32),
            dma((RING,)), dma((NCH + 2,)),
            dma((3 * NCH,)), dma((3 * NCH,)), dma((3 * NCH,)), dma((3 * NCH,)), dma((3 * NCH,)), dma((3 * NCH,)),
            dma((3, NCH)), dma((3, NCH)), dma((1,)), dma((1,)),
            dma((2,)), dma((2,)), dma((4,)), dma((4,)), dma((4,)), dma((8,)),
            dma((3,)), dma((3,)), dma((3,)), dma((3,)), dma((7,)), dma((7,)), dma((NCH,)), dma((NCH,)), dma((NCH,)), pltpu.VMEM((3, 4096), jnp.int32),
        ],
        compiler_params=pltpu.CompilerParams(collective_id=0, has_side_effects=True, vmem_limit_bytes=67043328),
        name="propagate",
    )(mask, eu0, ei0, tri)


def _lookup_kernel(uid, pid, nid, tri, items, items_p, users, part, out_i, out_u, it, ut, pp, pn):
    c = lax.axis_index("col")
    r = lax.axis_index("row")
    k = r % 2
    out_i[...] = items[...]
    out_u[...] = users[2 * r + c]
    for src, at in ((items, k * QUART), (items_p, (1 - k) * QUART)):
        for i in range(QUART // 512):
            rows = pl.ds(pl.multiple_of(at + i * 512, 512), 512)
            it[rows, :EMB] = src[:, i * 512:(i + 1) * 512].astype(F32).T
    for i in range(8):
        ut[i * HALF:(i + 1) * HALF, :EMB] = users[i].astype(F32).T

    @pl.loop(0, 2048 // 64)
    def _(i):
        for w in range(64):
            t = i * 64 + w
            g = k * 2048 + t
            u = ut[pl.ds(uid[g], 1), :]
            pp[pl.ds(t, 1), :] = u * it[pl.ds(pid[g], 1), :]
            pn[pl.ds(t, 1), :] = u * it[pl.ds(nid[g], 1), :]

    @pl.loop(0, 4)
    def _(i):
        for w in range(4):
            at = i * 4 + w
            rows = pl.ds(pl.multiple_of(at * 128, 128), 128)
            cols = pl.ds(pl.multiple_of(k * 2048 + at * 128, 128), 128)
            sp = jnp.sum(pp[rows, :].T[:EMB], axis=0, keepdims=True)
            sn = jnp.sum(pn[rows, :].T[:EMB], axis=0, keepdims=True)
            own_p = tri[1:2, cols] // (2 * QUART) == 2 * c + r // 2
            own_n = tri[2:3, cols] // (2 * QUART) == 2 * c + r // 2
            part[pl.ds(at, 1), :] = jnp.where(own_p, sp, 0.0) - jnp.where(own_n, sn, 0.0)


def _lookup(ids, tri, items, items_p, users):
    vmem = pl.BlockSpec(memory_space=pltpu.VMEM)
    smem = pl.BlockSpec(memory_space=pltpu.SMEM)
    return pl.pallas_call(
        _lookup_kernel,
        out_shape=(jax.ShapeDtypeStruct((16, 128), F32), jax.ShapeDtypeStruct((EMB, QUART), BF),
                   jax.ShapeDtypeStruct((EMB, HALF), BF)),
        in_specs=[smem, smem, smem, vmem, vmem, vmem, vmem],
        out_specs=(vmem, vmem, vmem),
        scratch_shapes=[pltpu.VMEM((2 * QUART, 128), F32), pltpu.VMEM((4096, 128), F32),
                        pltpu.VMEM((2048, 128), F32), pltpu.VMEM((2048, 128), F32)],
        name="lookup",
    )(*[i.reshape(4096) for i in ids], tri, items, items_p, users)


def _loss_kernel(part_in, out, got, part, s_sem, r_sem):
    c = lax.axis_index("col")
    r = lax.axis_index("row")
    me = 2 * r + c
    load = pltpu.make_async_copy(part_in, part, s_sem.at[0])
    load.start()
    barrier = pltpu.get_barrier_semaphore()
    for cc in range(2):
        for rr in range(4):
            pl.semaphore_signal(barrier, inc=1, device_id=(cc, rr), device_id_type=MESH)
    pl.semaphore_wait(barrier, 8)
    load.wait()

    def copy(i, slot):
        dr, dc = i // 2, i % 2
        return pltpu.make_async_remote_copy(
            src_ref=part, dst_ref=got.at[slot], send_sem=s_sem.at[i], recv_sem=r_sem.at[i],
            device_id=((c + dc) % 2, (r + dr) % 4), device_id_type=MESH)

    def sender(i):
        return 2 * ((r + 4 - i // 2) % 4) + (c + i % 2) % 2

    for i in range(1, 8):
        copy(i, me).start()
    got[me] = part[...]
    for i in range(1, 8):
        copy(i, sender(i)).wait()
    for h in range(2):
        m = (got[2 * h] + got[2 * h + 1]) + (got[2 * h + 4] + got[2 * h + 5])
        out[h * 16:(h + 1) * 16, :] = jnp.maximum(-m, 0.0) + jnp.log1p(jnp.exp(-jnp.abs(m)))


def _loss(part):
    vmem = pl.BlockSpec(memory_space=pltpu.VMEM)
    return pl.pallas_call(
        _loss_kernel,
        out_shape=jax.ShapeDtypeStruct((32, 128), F32),
        in_specs=[pl.BlockSpec(memory_space=pl.ANY)],
        out_specs=vmem,
        scratch_shapes=[pltpu.VMEM((8, 16, 128), F32), pltpu.VMEM((16, 128), F32), pltpu.SemaphoreType.DMA((8,)), pltpu.SemaphoreType.DMA((8,))],
        compiler_params=pltpu.CompilerParams(collective_id=1, has_side_effects=True),
        name="loss",
    )(part)


def solution(mesh):
    def device_body(mask_blk, user_shard, item_shard, triples):
        tri = triples.T
        out_it, par_it, users, *ids = _main(mask_blk, user_shard.T, item_shard.T, tri)
        part, out_it, out_ut = _lookup(ids, tri, out_it, par_it, users)
        bpr_loss = _loss(part).reshape(4096)
        return out_ut.T, out_it.T, bpr_loss

    return jax.shard_map(
        device_body,
        mesh=mesh,
        in_specs=(P("row", "col"), P(("row", "col"), None), P(("col", "row"), None), P()),
        out_specs=(P(("row", "col"), None), P(("col", "row"), None), P()),
        check_vma=False,
    )
```
